8 devices in a mesh: rep: 2 (over y, z), dp: 4 (over x, core).
Axes of the slice: x: 2, y: 2, z: 1, core: 2. Of those that a mesh axis runs over, the one named last changes fastest.
Arguments:
- x: bfloat16 [8, 2048, 1152], P(('rep', 'dp')), parts along dimension 0
- dy: bfloat16 [8, 2048, 1152], P(('rep', 'dp')), parts along dimension 0
- w_gate: bfloat16 [2, 1152, 4608], replicated
- w_up: bfloat16 [2, 1152, 4608], replicated
- w_down: bfloat16 [2, 4608, 1152], replicated
- m_w_gate: float32 [2, 1152, 4608], P(None, 'dp')
- m_w_up: float32 [2, 1152, 4608], P(None, 'dp')
- m_w_down: float32 [2, 4608, 1152], P(None, 'dp')
- v_w_gate: float32 [2, 1152, 4608], P(None, 'dp')
- v_w_up: float32 [2, 1152, 4608], P(None, 'dp')
- v_w_down: float32 [2, 4608, 1152], P(None, 'dp')
Outputs:
- output 1: bfloat16 [4, 1152, 4608], P('rep'), parts along dimension 0
- output 2: bfloat16 [4, 1152, 4608], P('rep'), parts along dimension 0
- output 3: bfloat16 [4, 4608, 1152], P('rep'), parts along dimension 0
- output 4: float32 [4, 1152, 4608], P('rep', 'dp'), parts along dimension 0
- output 5: float32 [4, 1152, 4608], P('rep', 'dp'), parts along dimension 0
- output 6: float32 [4, 4608, 1152], P('rep', 'dp'), parts along dimension 0
- output 7: float32 [4, 1152, 4608], P('rep', 'dp'), parts along dimension 0
- output 8: float32 [4, 1152, 4608], P('rep', 'dp'), parts along dimension 0
- output 9: float32 [4, 4608, 1152], P('rep', 'dp'), parts along dimension 0
There are 2 independent parts. The reference program is written for one: setup_inputs(seed, part) draws one part's arguments, and reference() takes and returns one part's arrays. A program takes and returns all parts, laid end to end along the dimension named above; an argument that names none is the same for every part.
All inputs are finite; a program needn't handle non-finite values.
Results may differ from the reference program's by a relative error of at most 0.022.
Values are sent between devices in bfloat16 or wider.
A program may use at most 2 GiB of HBM per device.

```python
import jax
import jax.numpy as jnp
from jax import lax

SEQUENCES = 4
TOKENS = 2048
D = 1152
FF = 4608
LAYERS = 2
NAMES = ("w_gate", "w_up", "w_down")
SHAPES = {"w_gate": (LAYERS, D, FF), "w_up": (LAYERS, D, FF), "w_down": (LAYERS, FF, D)}


def bump(key, n, height):
    away = (jnp.arange(n, dtype=jnp.int32) - jax.random.randint(key, (), 0, n, jnp.int32)) % n
    return jnp.where(away < n // 8, height, 1.0)


def together(key, own, strength):
    shared = jax.random.normal(key, own.shape[1:], jnp.float32)
    return (own + strength * shared) * lax.rsqrt(1 + strength * strength)


def setup_inputs(seed: int = 0, part: int = 0) -> dict:
    kx, kdy, ka, kb, kz, kf, kh, kl, *keys = jax.random.split(jax.random.key(seed), 8 + 3 * len(NAMES))
    kx, kdy, ka, kb = (jax.random.fold_in(k, part) for k in (kx, kdy, ka, kb))
    kw, km, kv = (keys[i::3] for i in range(3))
    shape = (SEQUENCES, TOKENS, D)
    much_x, much_dy = jax.random.uniform(kz, (2,), jnp.float32, 0.0, 1.0)
    loud = 2.0 ** jax.random.uniform(jax.random.fold_in(kz, 1), (), jnp.float32, -1.0, 2.0)
    layers = 2.0 ** jax.random.uniform(kl, (LAYERS, 1, 1), jnp.float32, -1.0, 1.0)
    x = together(ka, jax.random.normal(kx, shape, jnp.float32), much_x) * bump(kf, D, 4.0)
    dy = together(kb, jax.random.normal(kdy, shape, jnp.float32), much_dy)
    drawn = {"x": x.astype(jnp.bfloat16), "dy": (loud * dy * (SEQUENCES * TOKENS) ** -0.5).astype(jnp.bfloat16)}
    for key, name in zip(kw, NAMES, strict=True):
        w = jax.random.normal(key, SHAPES[name], jnp.float32) * SHAPES[name][1] ** -0.5
        drawn[name] = (w * {"w_gate": 1.0, "w_up": bump(kh, FF, 4.0), "w_down": layers}[name]).astype(jnp.bfloat16)
    for key, name in zip(km, NAMES, strict=True):
        drawn[f"m_{name}"] = 0.1 * jax.random.normal(key, SHAPES[name], jnp.float32)
    for key, name in zip(kv, NAMES, strict=True):
        drawn[f"v_{name}"] = jax.random.uniform(key, SHAPES[name], jnp.float32, 0.005, 0.015)
    return drawn


def matmul(a, w):
    return jnp.dot(a, w, preferred_element_type=jnp.float32).astype(jnp.bfloat16)


def normed(h):
    wide = h.astype(jnp.float32)
    scale = lax.rsqrt(jnp.mean(wide**2, -1, keepdims=True) + 1e-6)
    return (wide * scale).astype(jnp.bfloat16)


def layer(h, w):
    a = normed(h)
    gate = jnp.dot(a, w["w_gate"], preferred_element_type=jnp.float32)
    up = jnp.dot(a, w["w_up"], preferred_element_type=jnp.float32)
    return h + matmul((jax.nn.silu(gate) * up).astype(jnp.bfloat16), w["w_down"])


def adamw(w, m, v, g):
    m = 0.9 * m + 0.1 * g
    v = 0.95 * v + 0.05 * g * g
    step = m * lax.rsqrt(v + 1e-8) + 0.1 * w
    return (w - 0.02 * step).astype(jnp.bfloat16), m, v


def stack(weights, h):
    return lax.scan(lambda h, w: (layer(h, w), None), h, weights)[0]


def reference(x, dy, w_gate, w_up, w_down, m_w_gate, m_w_up, m_w_down, v_w_gate, v_w_up, v_w_down):
    weights = dict(zip(NAMES, (w_gate, w_up, w_down), strict=True))

    def take(so_far, sequence):
        h, by_y = sequence
        _, back = jax.vjp(lambda w: stack(w, h), weights)
        return jax.tree.map(lambda total, term: total + term.astype(jnp.float32), so_far, back(by_y)[0]), None

    none_yet = {name: jnp.zeros(w.shape, jnp.float32) for name, w in weights.items()}
    by_weights, _ = lax.scan(take, none_yet, (x, dy))
    gradients = [by_weights[name].astype(jnp.bfloat16).astype(jnp.float32) for name in NAMES]
    new = [
        adamw(w.astype(jnp.float32), m, v, g)
        for w, m, v, g in zip((w_gate, w_up, w_down), (m_w_gate, m_w_up, m_w_down), (v_w_gate, v_w_up, v_w_down), gradients, strict=True)
    ]
    return tuple(one[which] for which in range(3) for one in new)
```

```python
import jax
import jax.numpy as jnp
from jax import lax
from jax.experimental import pallas as pl
from jax.experimental.pallas import tpu as pltpu
from jax.sharding import PartitionSpec as P


f32, bf16 = jnp.float32, jnp.bfloat16
T, D, F = 2048, 1152, 4608
TT = 2 * T
HALF = F // 2
BM, BN = 1024, 768
NF, NH = F // BN, HALF // BN
RS, CS = 512, 256
QD, QF = D // 4, F // 4
ANY = pl.BlockSpec(memory_space=pl.ANY)
TOKEN = jax.ShapeDtypeStruct((8, 128), jnp.int32)
NT = (((1,), (1,)), ((), ()))
TN = (((0,), (0,)), ((), ()))

OVER_X = [(0, 2), (1, 3), (2, 0), (3, 1)]
OVER_CORE = [(0, 1), (1, 0), (2, 3), (3, 2)]


def over(array, pairs):
    return lax.ppermute(array, "dp", pairs)


def sigmoid(g):
    return 0.5 * jnp.tanh(0.5 * g) + 0.5


def dot(a, b):
    return jnp.dot(a, b, preferred_element_type=f32)


def call(body, place, after, ins, outs, grid, scratch=(), flops=0, moved=0):
    arrays = [a for a, _ in ins]
    specs = [s for _, s in ins]
    aliases = {}
    held = [(k, buffer) for k, (_, _, buffer) in enumerate(outs) if buffer is not None]
    for n, (k, buffer) in enumerate(held):
        aliases[1 + len(arrays) + n] = k
    arrays += [buffer for _, buffer in held]
    specs += [ANY] * len(held)
    if after is not None:
        arrays.append(after)
        specs.append(ANY)
    skip = len(arrays) - len(ins)

    def kernel(place_ref, *refs):
        refs, rest = refs[: len(ins)], refs[len(ins) + skip :]
        token = rest[len(outs)]
        token[...] = jnp.zeros_like(token)
        body(place_ref, *refs, *rest[: len(outs)], *rest[len(outs) + 1 :])

    result = pl.pallas_call(
        kernel,
        grid_spec=pltpu.PrefetchScalarGridSpec(
            num_scalar_prefetch=1,
            grid=grid,
            in_specs=specs,
            out_specs=[s for _, s, _ in outs] + [pl.BlockSpec((8, 128), lambda *_: (0, 0))],
            scratch_shapes=scratch,
        ),
        out_shape=[o for o, _, _ in outs] + [TOKEN],
        input_output_aliases=aliases,
        cost_estimate=pl.CostEstimate(flops=flops, bytes_accessed=moved, transcendentals=0),
        compiler_params=pltpu.CompilerParams(vmem_limit_bytes=63 << 20),
    )(place, *arrays)
    return result[:-1], result[-1]


def shaped(*shape, dtype=bf16):
    return jax.ShapeDtypeStruct(shape, dtype)


def normalise(h, a_s, aT):
    def rows_of(i, _):
        rows = pl.ds(pl.multiple_of(i * 256, 256), 256)
        wide = h[rows, :].astype(f32)
        scale = lax.rsqrt(jnp.mean(wide * wide, -1, keepdims=True) + 1e-6)
        a = (wide * scale).astype(bf16)
        a_s[rows, :] = a
        if aT is not None:
            aT[:, rows] = a.T
        return 0

    lax.fori_loop(0, h.shape[0] // 256, rows_of, 0)


def forward0(place, after, first, x, w_gate, w_up, w_down, held):
    rows = x.shape[0]

    def tile(j, place):
        return jnp.where(j < NH, place[0] * NH + j, (1 - place[0]) * NH + j - NH)

    def body(place, x, wg, wu, wd, g_o, u_o, hid_o, aT_o, h_o, a_s, acc, hs):
        j = pl.program_id(1)

        @pl.when(j == 0)
        def _():
            normalise(x, a_s, aT_o)

        for r in range(0, BM, RS):
            r = slice(r, r + RS)
            a = a_s[r, :]
            for c in range(0, BN, CS):
                c = slice(c, c + CS)
                g, u = dot(a, wg[:, c]), dot(a, wu[:, c])
                g_o[r, c] = g
                u_o[r, c] = u
                hs[r, c] = (g * sigmoid(g) * u).astype(bf16)
            acc[r, :] = jnp.where(j == 0, 0.0, acc[r, :]) + dot(hs[r, :], wd[...])

        @pl.when(j < NH)
        def _():
            hid_o[...] = hs[...]

        @pl.when(j == NF - 1)
        def _():
            def rows_of(i, _):
                rows = pl.ds(pl.multiple_of(i * 256, 256), 256)
                h_o[rows, :] = x[rows, :] + acc[rows, :].astype(bf16)
                return 0

            lax.fori_loop(0, BM // 256, rows_of, 0)

    wide = pl.BlockSpec((BM, BN), lambda i, j, p: (first + i, tile(j, p)))
    into = pl.BlockSpec((None, D, BN), lambda i, j, p: (0, 0, tile(j, p)))
    return call(
        body,
        place,
        after,
        [
            (x, pl.BlockSpec((BM, D), lambda i, j, p: (i, 0))),
            (w_gate, into),
            (w_up, into),
            (w_down, pl.BlockSpec((None, BN, D), lambda i, j, p: (0, tile(j, p), 0))),
        ],
        [
            (shaped(TT, F, dtype=f32), wide, held[0]),
            (shaped(TT, F, dtype=f32), wide, held[1]),
            (shaped(TT, HALF), pl.BlockSpec((BM, BN), lambda i, j, p: (first + i, jnp.minimum(j, NH - 1))), held[2]),
            (shaped(D, TT), pl.BlockSpec((D, BM), lambda i, j, p: (0, first + i)), held[3]),
            (shaped(TT, D), pl.BlockSpec((BM, D), lambda i, j, p: (first + i, 0)), held[4]),
        ],
        (rows // BM, NF),
        [pltpu.VMEM((BM, D), bf16), pltpu.VMEM((BM, D), f32), pltpu.VMEM((BM, BN), bf16)],
        flops=6 * rows * D * F,
        moved=rows * F * 9,
    )


def both1(place, after, first, own, h, dy, w_gate, w_up, w_down, held):
    rows = dy.shape[0]

    def tile(j, place):
        return (place[0] if own else 1 - place[0]) * NH + j

    def body(place, h, dy, wg, wu, wd, *refs):
        if own:
            dgu_o, hid_o, aT_o, a_s = refs
        else:
            (dgu_o, a_s), hid_o, aT_o = refs, None, None
        j = pl.program_id(1)

        @pl.when(j == 0)
        def _():
            normalise(h, a_s, aT_o)

        for r in range(0, BM, RS):
            r = slice(r, r + RS)
            a = a_s[r, :]
            for c in range(0, BN, CS):
                c = slice(c, c + CS)
                g, u = dot(a, wg[:, c]), dot(a, wu[:, c])
                back = lax.dot_general(dy[r, :], wd[c, :], NT, preferred_element_type=f32).astype(bf16).astype(f32)
                s = sigmoid(g)
                silu = g * s
                if own:
                    hid_o[r, c] = (silu * u).astype(bf16)
                dgu_o[0, r, c] = (back * u * (s + silu * (1 - s))).astype(bf16)
                dgu_o[1, r, c] = (back * silu).astype(bf16)

    into = pl.BlockSpec((None, D, BN), lambda i, j, p: (1, 0, tile(j, p)))
    outs = [(shaped(2, TT, F), pl.BlockSpec((2, BM, BN), lambda i, j, p: (0, first + i, tile(j, p))), held[0])]
    if own:
        outs += [
            (shaped(TT, HALF), pl.BlockSpec((BM, BN), lambda i, j, p: (first + i, j)), held[1]),
            (shaped(D, TT), pl.BlockSpec((D, BM), lambda i, j, p: (0, first + i)), held[2]),
        ]
    return call(
        body,
        place,
        after,
        [
            (h, pl.BlockSpec((BM, D), lambda i, j, p: (first + i, 0))),
            (dy, pl.BlockSpec((BM, D), lambda i, j, p: (i, 0))),
            (w_gate, into),
            (w_up, into),
            (w_down, pl.BlockSpec((None, BN, D), lambda i, j, p: (1, tile(j, p), 0))),
        ],
        outs,
        (rows // BM, NH),
        [pltpu.VMEM((BM, D), bf16)],
        flops=3 * rows * D * F,
        moved=rows * F * 3,
    )


def back1(place, after, first, dgu, dy, h, w_gate, w_up, held):
    rows = dy.shape[0]

    def body(place, dgu, wg, wu, h, dy, o, acc):
        j = pl.program_id(1)
        for r in range(0, BM, RS):
            r = slice(r, r + RS)
            for which, w in enumerate((wg, wu)):
                new = lax.dot_general(dgu[which, r, :], w[...], NT, preferred_element_type=f32)
                acc[which, r, :] = jnp.where(j == 0, 0.0, acc[which, r, :]) + new

        @pl.when(j == NF - 1)
        def _():
            def rows_of(i, _):
                rows = pl.ds(pl.multiple_of(i * 256, 256), 256)
                da = (acc[0, rows, :].astype(bf16) + acc[1, rows, :].astype(bf16)).astype(f32)
                wide = h[rows, :].astype(f32)
                scale = lax.rsqrt(jnp.mean(wide * wide, -1, keepdims=True) + 1e-6)
                along = jnp.mean(da * wide, -1, keepdims=True)
                dwide = (da * scale - wide * (along * scale * scale * scale)).astype(bf16)
                o[rows, :] = dy[rows, :] + dwide
                return 0

            lax.fori_loop(0, BM // 256, rows_of, 0)

    into = pl.BlockSpec((None, D, BN), lambda i, j, p: (1, 0, j))
    return call(
        body,
        place,
        after,
        [
            (dgu, pl.BlockSpec((2, BM, BN), lambda i, j, p: (0, first + i, j))),
            (w_gate, into),
            (w_up, into),
            (h, pl.BlockSpec((BM, D), lambda i, j, p: (first + i, 0))),
            (dy, pl.BlockSpec((BM, D), lambda i, j, p: (i, 0))),
        ],
        [(shaped(TT, D), pl.BlockSpec((BM, D), lambda i, j, p: (first + i, 0)), held)],
        (rows // BM, NF),
        [pltpu.VMEM((2, BM, D), f32)],
        flops=4 * rows * D * F,
        moved=rows * F * 4,
    )


def back0(place, after, own, dh, gate, up, w_down, held):
    def tile(j, place):
        return (place[0] if own else 1 - place[0]) * NH + j

    def body(place, dh, g_r, u_r, wd, dgu_o):
        for r in range(0, BM, RS):
            r = slice(r, r + RS)
            for c in range(0, BN, CS):
                c = slice(c, c + CS)
                back = lax.dot_general(dh[r, :], wd[c, :], NT, preferred_element_type=f32).astype(bf16).astype(f32)
                g, u = g_r[r, c], u_r[r, c]
                s = sigmoid(g)
                silu = g * s
                dgu_o[0, r, c] = (back * u * (s + silu * (1 - s))).astype(bf16)
                dgu_o[1, r, c] = (back * silu).astype(bf16)

    wide = pl.BlockSpec((BM, BN), lambda i, j, p: (i, tile(j, p)))
    return call(
        body,
        place,
        after,
        [
            (dh, pl.BlockSpec((BM, D), lambda i, j, p: (i, 0))),
            (gate, wide),
            (up, wide),
            (w_down, pl.BlockSpec((None, BN, D), lambda i, j, p: (0, tile(j, p), 0))),
        ],
        [(shaped(2, TT, F), pl.BlockSpec((2, BM, BN), lambda i, j, p: (0, i, tile(j, p))), held)],
        (TT // BM, NH),
        flops=TT * D * F,
        moved=TT * F * 6,
    )


def grad_down(place, after, hidden, back):
    rows = 384
    n = QF // rows
    parts = [b.shape[0] for b in back]

    def tile(i, place):
        return jnp.where(i < n, place[1] * n + i, (1 - place[1]) * n + i - n)

    def body(place, hidden, *refs):
        back, (own, out) = refs[:-2], refs[-2:]
        i = pl.program_id(0)
        total = None
        at = 0
        for b, size in zip(back, parts, strict=True):
            term = lax.dot_general(hidden[at : at + size, :], b[...], TN, preferred_element_type=f32)
            total = term if total is None else total + term
            at += size

        @pl.when(i < n)
        def _():
            own[...] = total

        @pl.when(i >= n)
        def _():
            out[...] = total.astype(bf16)

    return call(
        body,
        place,
        after,
        [(hidden, pl.BlockSpec((TT, rows), lambda i, p: (0, tile(i, p))))]
        + [(b, pl.BlockSpec((b.shape[0], D), lambda i, p: (0, 0), pipeline_mode=pl.Buffered(1))) for b in back],
        [
            (shaped(QF, D, dtype=f32), pl.BlockSpec((rows, D), lambda i, p: (jnp.minimum(i, n - 1), 0)), None),
            (shaped(QF, D), pl.BlockSpec((rows, D), lambda i, p: (jnp.maximum(i - n, 0), 0)), None),
        ],
        (2 * n,),
        flops=2 * TT * D * HALF,
        moved=TT * HALF * 2,
    )


def grad_into(place, after, own_half, aT, dgu):
    def tile(j, place):
        return (place[0] if own_half else 1 - place[0]) * NH + j

    def body(place, aT, dgu, own, out, total):
        total[...] = dot(aT[...], dgu[...])
        own[...] = total[pl.ds(pl.multiple_of(place[1] * QD, QD), QD), :]
        out[...] = total[pl.ds(pl.multiple_of((1 - place[1]) * QD, QD), QD), :].astype(bf16)

    block = pl.BlockSpec((None, QD, BN), lambda k, j, p: (k, 0, j))
    return call(
        body,
        place,
        after,
        [
            (aT, pl.BlockSpec((2 * QD, TT), lambda k, j, p: (p[0], 0), pipeline_mode=pl.Buffered(1))),
            (dgu, pl.BlockSpec((None, TT, BN), lambda k, j, p: (k, 0, tile(j, p)))),
        ],
        [(shaped(2, QD, HALF, dtype=f32), block, None), (shaped(2, QD, HALF), block, None)],
        (2, NH),
        [pltpu.VMEM((2 * QD, BN), f32)],
        flops=2 * TT * D * HALF,
        moved=TT * HALF * 4,
    )


def adamw(g, w, m, v):
    g = g.astype(bf16).astype(f32)
    m = 0.9 * m + 0.1 * g
    v = 0.95 * v + 0.05 * g * g
    return (w - 0.02 * (m * lax.rsqrt(v + 1e-8) + 0.1 * w)).astype(bf16), m, v


def step_down(place, after, layer, own, came, w, m, v, held):
    rows = 192

    def body(place, own, came, w, m, v, nw_o, m_o, v_o):
        nw_o[...], m_o[...], v_o[...] = adamw(own[...] + came[...].astype(f32), w[...].astype(f32), m[...], v[...])

    n = QF // rows
    block = pl.BlockSpec((rows, D), lambda i, p: (i, 0))
    kept = pl.BlockSpec((None, rows, D), lambda i, p: (layer, i, 0))
    return call(
        body,
        place,
        after,
        [
            (own, block),
            (came, block),
            (w, pl.BlockSpec((None, rows, D), lambda i, p: (layer, (2 * p[0] + p[1]) * n + i, 0))),
            (m, kept),
            (v, kept),
        ],
        [(shaped(QF, D), block, None), (shaped(2, QF, D, dtype=f32), kept, held[0]), (shaped(2, QF, D, dtype=f32), kept, held[1])],
        (n,),
        flops=QF * D * 10,
        moved=QF * D * 26,
    )


def step_into(place, after, layer, own_half, k, own, came, w, m, v, held):
    def body(place, own, came, w, m, v, nw_o, m_o, v_o):
        nw_o[...], m_o[...], v_o[...] = adamw(own[...] + came[...].astype(f32), w[...].astype(f32), m[...], v[...])

    def tile(j, place):
        return (place[0] if own_half else 1 - place[0]) * NH + j

    block = pl.BlockSpec((None, QD, BN), lambda j, p: (k, 0, j))
    kept = pl.BlockSpec((None, QD, BN), lambda j, p: (layer, 0, tile(j, p)))
    return call(
        body,
        place,
        after,
        [
            (own, block),
            (came, block),
            (w, pl.BlockSpec((None, QD, BN), lambda j, p: (layer, 2 * p[0] + p[1], tile(j, p)))),
            (m, kept),
            (v, kept),
        ],
        [
            (shaped(QD, HALF), pl.BlockSpec((QD, BN), lambda j, p: (0, j)), None),
            (shaped(2, QD, F, dtype=f32), kept, held[0]),
            (shaped(2, QD, F, dtype=f32), kept, held[1]),
        ],
        (NH,),
        flops=QD * HALF * 10,
        moved=QD * HALF * 26,
    )


def gathered(place, after, block, blocks, spec_in, spec_out, out, held):
    n = spec_in[0]

    def body(place, *refs):
        sources, o = refs[:4], refs[4]
        r = pl.program_id(0)
        for k, source in enumerate(sources):

            @pl.when(r == k)
            def _(source=source):
                o[...] = source[...]

    def source_spec(k):
        return pl.BlockSpec(block, lambda r, j, p: spec_in[1](jnp.where(r == k, j, jnp.where(r < k, 0, n - 1))))

    return call(
        body,
        place,
        after,
        [(b, source_spec(k)) for k, b in enumerate(blocks)],
        [(out, pl.BlockSpec((None,) + block, lambda r, j, p: spec_out(jnp.bitwise_xor(2 * p[0] + p[1], r), j, p)), held)],
        (4, n),
        moved=4 * blocks[0].size * 4,
        flops=blocks[0].size,
    )


def gather_down(place, after, layer, blocks, held):
    rows = 384
    n = QF // rows
    return gathered(
        place, after, (rows, D), blocks, (n, lambda j: (j, 0)), lambda d, j, p: (layer, d * n + j, 0), shaped(2, F, D), held
    )


def gather_into(place, after, layer, blocks, flip, held):
    def spec_out(d, j, p):
        half = jnp.bitwise_xor(d // 2, flip)
        return (layer, d, half * NH + j)

    return gathered(place, after, (QD, BN), blocks, (NH, lambda j: (0, j)), spec_out, shaped(2, D, F), held)


def spread(new):
    far = over(new, OVER_X)
    near = over(new, OVER_CORE)
    return [new, near, far, over(far, OVER_CORE)]


def whole_step(x, dy, w_gate, w_up, w_down, m_gate, m_up, m_down, v_gate, v_up, v_down):
    d = lax.axis_index("dp")
    place = jnp.stack([d // 2, d % 2]).astype(jnp.int32)
    x, dy = x[0], dy[0]
    x_far = over(x, OVER_X)
    dy_far = over(dy, OVER_X)
    per = T // BM

    ws0 = (w_gate, w_up, w_down)
    one, t = forward0(place, None, 0, x, *ws0, [None] * 5)
    (gate, up, hid0, aT0, h), t = forward0(place, t, per, x_far, *ws0, one)

    one, t = both1(place, t, 0, True, h, dy, *ws0, [None] * 3)
    (dgu, hid1, aT1), t = both1(place, t, per, True, h, dy_far, *ws0, one)

    down1, t = grad_down(place, t, hid1, (dy, dy_far))
    down1_came = over(down1[1], OVER_CORE)
    into1a, t = grad_into(place, t, True, aT1, dgu)
    into1a_came = over(into1a[1], OVER_CORE)

    (n_down1, *mv_down), t = step_down(place, t, 1, down1[0], down1_came, w_down, m_down, v_down, (None, None))
    s_down1 = spread(n_down1)

    (dgu,), t = both1(place, t, 0, False, h, dy, *ws0, [dgu])

    def steps_into(t, layer, own_half, grads, came, mv_gate, mv_up):
        (new_gate, *mv_gate), t = step_into(place, t, layer, own_half, 0, grads[0], came, w_gate, m_gate, v_gate, mv_gate)
        (new_up, *mv_up), t = step_into(place, t, layer, own_half, 1, grads[0], came, w_up, m_up, v_up, mv_up)
        return t, spread(new_gate), spread(new_up), mv_gate, mv_up

    t, s_gate1a, s_up1a, mv_gate, mv_up = steps_into(t, 1, True, into1a, into1a_came, (None, None), (None, None))
    (dgu,), t = both1(place, t, per, False, h, dy_far, *ws0, [dgu])

    into1b, t = grad_into(place, t, False, aT1, dgu)
    into1b_came = over(into1b[1], OVER_CORE)
    (dh,), t = back1(place, t, 0, dgu, dy, h, w_gate, w_up, None)
    t, s_gate1b, s_up1b, mv_gate, mv_up = steps_into(t, 1, False, into1b, into1b_came, mv_gate, mv_up)
    (dh,), t = back1(place, t, per, dgu, dy_far, h, w_gate, w_up, dh)

    down0, t = grad_down(place, t, hid0, (dh,))
    down0_came = over(down0[1], OVER_CORE)
    (dgu0,), t = back0(place, t, True, dh, gate, up, w_down, None)
    (n_down0, *mv_down), t = step_down(place, t, 0, down0[0], down0_came, w_down, m_down, v_down, mv_down)
    s_down0 = spread(n_down0)

    into0a, t = grad_into(place, t, True, aT0, dgu0)
    into0a_came = over(into0a[1], OVER_CORE)
    (dgu0,), t = back0(place, t, False, dh, gate, up, w_down, dgu0)
    t, s_gate0a, s_up0a, mv_gate, mv_up = steps_into(t, 0, True, into0a, into0a_came, mv_gate, mv_up)

    into0b, t = grad_into(place, t, False, aT0, dgu0)
    into0b_came = over(into0b[1], OVER_CORE)
    (o_down,), t = gather_down(place, t, 1, s_down1, None)
    (o_gate,), t = gather_into(place, t, 1, s_gate1a, 0, None)
    t, s_gate0b, s_up0b, mv_gate, mv_up = steps_into(t, 0, False, into0b, into0b_came, mv_gate, mv_up)
    (o_up,), t = gather_into(place, t, 1, s_up1a, 0, None)
    (o_gate,), t = gather_into(place, t, 1, s_gate1b, 1, o_gate)
    (o_up,), t = gather_into(place, t, 1, s_up1b, 1, o_up)
    (o_down,), t = gather_down(place, t, 0, s_down0, o_down)
    (o_gate,), t = gather_into(place, t, 0, s_gate0a, 0, o_gate)
    (o_up,), t = gather_into(place, t, 0, s_up0a, 0, o_up)
    (o_gate,), t = gather_into(place, t, 0, s_gate0b, 1, o_gate)
    (o_up,), t = gather_into(place, t, 0, s_up0b, 1, o_up)
    return o_gate, o_up, o_down, mv_gate[0], mv_up[0], mv_down[0], mv_gate[1], mv_up[1], mv_down[1]


def solution(mesh):
    sequences, whole = P(("rep", "dp"), None, None), P(None, None, None)
    block, group, own = P(None, "dp", None), P("rep", None, None), P("rep", "dp", None)
    return jax.shard_map(
        whole_step,
        mesh=mesh,
        in_specs=(sequences,) * 2 + (whole,) * 3 + (block,) * 6,
        out_specs=(group,) * 3 + (own,) * 6,
        check_vma=False,
    )
```

```python
import functools

import jax
import jax.numpy as jnp
from jax import lax
from jax.experimental import pallas as pl
from jax.experimental.pallas import tpu as pltpu
from jax.sharding import PartitionSpec as P


f32, bf16 = jnp.float32, jnp.bfloat16
T, D, F = 2048, 1152, 4608
TT = 2 * T
HALF = F // 2
BM, BN = 1024, 768
NF, NH = F // BN, HALF // BN
RS, CS = 512, 256
NQ = 384
VMEM = 67043328
QD, QF = D // 4, F // 4
ANY = pl.BlockSpec(memory_space=pl.ANY)
TOKEN = jax.ShapeDtypeStruct((8, 128), jnp.int32)
NT = (((1,), (1,)), ((), ()))
TN = (((0,), (0,)), ((), ()))

OVER_X = [(d, d ^ 2) for d in range(4)]
OVER_CORE = [(d, d ^ 1) for d in range(4)]


def over(array, pairs):
    return lax.ppermute(array, "dp", pairs)


def sigmoid(g):
    return 0.5 * jnp.tanh(0.5 * g) + 0.5


def cuts(n, size):
    return [slice(at, at + size) for at in range(0, n, size)]


def added(first, total, new):
    return jnp.where(first, 0.0, total) + new


def gated(g, u, back):
    s = sigmoid(g)
    silu = g * s
    return (silu * u).astype(bf16), (back * u * (s + silu * (1 - s))).astype(bf16), (back * silu).astype(bf16)


def dot(a, b):
    return jnp.dot(a, b, preferred_element_type=f32)


def call(body, place, after, ins, outs, grid, scratch=(), jobs=()):
    bodies = [(body, len(ins), len(outs), len(scratch))] + [(job, len(i), len(o), len(s)) for i, o, job, s in jobs]
    ins = list(ins) + [one for i, _, _, _ in jobs for one in i]
    outs = list(outs) + [one for _, o, _, _ in jobs for one in o]
    scratch = list(scratch) + [one for _, _, _, s in jobs for one in s]
    arrays = [a for a, _ in ins]
    specs = [s for _, s in ins]
    aliases = {}
    held = [(k, buffer) for k, (_, _, buffer) in enumerate(outs) if buffer is not None]
    for n, (k, buffer) in enumerate(held):
        aliases[1 + len(arrays) + n] = k
    arrays += [buffer for _, buffer in held]
    specs += [ANY] * len(held)
    if after is not None:
        arrays.append(after)
        specs.append(ANY)
    skip = len(arrays) - len(ins)

    def kernel(place_ref, *refs):
        refs, rest = refs[: len(ins)], refs[len(ins) + skip :]
        results, token, own = rest[: len(outs)], rest[len(outs)], rest[len(outs) + 1 :]
        token[...] = jnp.zeros_like(token)
        parts = []
        at_in = at_out = at = 0
        for one, n_in, n_out, n in bodies:
            mine = (*refs[at_in : at_in + n_in], *results[at_out : at_out + n_out], *own[at : at + n])
            parts.append(functools.partial(one, place_ref, *mine))
            at_in, at_out, at = at_in + n_in, at_out + n_out, at + n
        for part, (one, *_) in zip(parts, bodies, strict=True):
            if getattr(one, "copies", False):
                part()
        last = [part() for part, (one, *_) in zip(parts, bodies, strict=True) if not getattr(one, "copies", False)]
        if last[0] is not None:
            last[0]()

    result = pl.pallas_call(
        kernel,
        grid_spec=pltpu.PrefetchScalarGridSpec(
            num_scalar_prefetch=1,
            grid=grid,
            in_specs=specs,
            out_specs=[s for _, s, _ in outs] + [pl.BlockSpec((8, 128), lambda *_: (0, 0))],
            scratch_shapes=scratch,
        ),
        out_shape=[o for o, _, _ in outs] + [TOKEN],
        input_output_aliases=aliases,
        cost_estimate=pl.CostEstimate(flops=T * D * F, bytes_accessed=T * D * F, transcendentals=0),
        compiler_params=pltpu.CompilerParams(vmem_limit_bytes=VMEM),
    )(place, *arrays)
    return result[:-1], result[-1]


def shaped(*shape, dtype=bf16):
    return jax.ShapeDtypeStruct(shape, dtype)


def normalise(h, a_s, aT):
    def rows_of(i, _):
        rows = pl.ds(pl.multiple_of(i * 256, 256), 256)
        wide = h[rows, :].astype(f32)
        scale = lax.rsqrt(jnp.mean(wide * wide, -1, keepdims=True) + 1e-6)
        a = (wide * scale).astype(bf16)
        a_s[rows, :] = a
        if aT is not None:
            aT[:, rows] = a.T
        return 0

    lax.fori_loop(0, h.shape[0] // 256, rows_of, 0)


def forward0(place, after, first, x, w_gate, w_up, w_down, held, whole):
    rows = x.shape[0]

    def tile(j, place):
        return jnp.where(j < NH, place[0] * NH + j, (1 - place[0]) * NH + j - NH)

    def body(place, x, wg, wu, *refs):
        if whole:
            wd, g_o, u_o, hid_o, aT_o, h_o, a1_o, aT1_o, a_s, hs, acc = refs
        else:
            g_o, u_o, hid_o, aT_o, a_s, hs = refs
        j = pl.program_id(1)

        @pl.when(j == 0)
        def _():
            normalise(x, a_s, aT_o)

        for r in cuts(BM, RS):
            a = a_s[r, :]
            for c in cuts(BN, CS):
                g, u = dot(a, wg[:, c]), dot(a, wu[:, c])
                g_o[r, c] = g
                u_o[r, c] = u
                hs[r, c] = (g * sigmoid(g) * u).astype(bf16)
            if whole:
                acc[r, :] = added(j == 0, acc[r, :], dot(hs[r, :], wd[...]))

        @pl.when(j < NH)
        def _():
            hid_o[...] = hs[...]

        if whole:

            @pl.when(j == NF - 1)
            def _():
                def rows_of(i, _):
                    rows = pl.ds(pl.multiple_of(i * 256, 256), 256)
                    h_o[rows, :] = x[rows, :] + acc[rows, :].astype(bf16)
                    return 0

                lax.fori_loop(0, BM // 256, rows_of, 0)
                normalise(h_o, a1_o, aT1_o)

    wide = pl.BlockSpec((BM, BN), lambda i, j, p: (first + i, tile(j, p)))
    into = pl.BlockSpec((None, D, BN), lambda i, j, p: (0, 0, tile(j, p)))
    plain = pl.BlockSpec((BM, D), lambda i, j, p: (i, 0))
    ins = [(x, plain), (w_gate, into), (w_up, into)]
    outs = [
        (shaped(TT, F, dtype=f32), wide, held[0]),
        (shaped(TT, F, dtype=f32), wide, held[1]),
        (shaped(TT, HALF), pl.BlockSpec((BM, BN), lambda i, j, p: (first + i, jnp.minimum(j, NH - 1))), held[2]),
        (shaped(D, TT), pl.BlockSpec((D, BM), lambda i, j, p: (0, first + i)), held[3]),
    ]
    scratch = [pltpu.VMEM((BM, D), bf16), pltpu.VMEM((BM, BN), bf16)]
    if whole:
        ins += [(w_down, pl.BlockSpec((None, BN, D), lambda i, j, p: (0, tile(j, p), 0)))]
        outs += [(shaped(T, D), plain, None), (shaped(T, D), plain, None)]
        outs += [(shaped(D, T), pl.BlockSpec((D, BM), lambda i, j, p: (0, i)), None)]
        scratch += [pltpu.VMEM((BM, D), f32)]
    return call(body, place, after, ins, outs, (rows // BM, NF), scratch)


def layer1(place, after, span, a1, aT, dy, w_gate, w_up, w_down, held):
    steps = T // BM
    first, stride, tiles = span
    t = first % NH
    rows = NQ if t == 1 else 2 * NQ

    def at(j):
        return first + stride * j

    def body(place, a1, aT, dy, wg, wu, wd, dgu_o, keep, out, down_keep, down_out, total, leaving, hid, down, down_leaving, sem):
        j, i = pl.program_id(0), pl.program_id(1)
        core = place[1]

        def mine(x, core):
            return pl.ds(pl.multiple_of((2 * x + core) * QD, QD), QD)

        def each(j, act):
            side = jnp.where(place[0] == at(j) // NH, 0, 1)
            columns = pl.ds(pl.multiple_of(j * BN, BN), BN)
            for x in range(2):
                act(pltpu.make_async_copy(total.at[:, mine(x, core), :], keep.at[:, x, :, columns], sem.at[x]))
            act(pltpu.make_async_copy(leaving, out.at[:, :, :, columns], sem.at[2]))
            for s in range(2):
                owner = (2 * t + s) // 3
                here, to = pl.ds(s * NQ, NQ), pl.ds(0 if t == 1 else s * NQ, NQ)

                @pl.when(core == owner)
                def _():
                    act(pltpu.make_async_copy(down.at[here, :], down_keep.at[side, to, :], sem.at[3 + s]))

                @pl.when(core != owner)
                def _():
                    act(pltpu.make_async_copy(down_leaving.at[here, :], down_out.at[side, to, :], sem.at[3 + s]))

        @pl.when((j > 0) & (i == 0))
        def _():
            each(j - 1, lambda copy: copy.wait())

        for r in cuts(BM, RS):
            a = a1[r, :]
            for c in cuts(BN, CS):
                g, u = dot(a, wg[:, c]), dot(a, wu[:, c])
                back = lax.dot_general(dy[r, :], wd[c, :], NT, preferred_element_type=f32).astype(bf16).astype(f32)
                hid[r, c], dgu_o[0, r, c], dgu_o[1, r, c] = gated(g, u, back)
        for k in range(2):
            total[k] = added(i == 0, total[k], dot(aT[...], dgu_o[k]))
        down[...] = added(i == 0, down[...], lax.dot_general(hid[...], dy[...], TN, preferred_element_type=f32))

        def last():
            @pl.when(i == steps - 1)
            def _():
                for x in range(2):
                    leaving[:, x] = total[:, mine(x, 1 - core), :].astype(bf16)
                down_leaving[...] = down[...].astype(bf16)
                each(j, lambda copy: copy.start())

            @pl.when((j == tiles - 1) & (i == steps - 1))
            def _():
                each(j, lambda copy: copy.wait())

        return last

    into = pl.BlockSpec((None, D, BN), lambda j, i, p: (1, 0, at(j)))
    plain = pl.BlockSpec((BM, D), lambda j, i, p: (i, 0))
    return call(
        body,
        place,
        after,
        [
            (a1, plain),
            (aT, pl.BlockSpec((D, BM), lambda j, i, p: (0, i))),
            (dy, plain),
            (w_gate, into),
            (w_up, into),
            (w_down, pl.BlockSpec((None, BN, D), lambda j, i, p: (1, at(j), 0))),
        ],
        [
            (shaped(2, T, F), pl.BlockSpec((2, BM, BN), lambda j, i, p: (0, i, at(j))), held[0]),
            (shaped(2, 2, QD, tiles * BN, dtype=f32), ANY, None),
            (shaped(2, 2, QD, tiles * BN), ANY, None),
            (shaped(2, rows, D, dtype=f32), ANY, held[1]),
            (shaped(2, rows, D), ANY, held[2]),
        ],
        (tiles, steps),
        [
            pltpu.VMEM((2, D, BN), f32),
            pltpu.VMEM((2, 2, QD, BN), bf16),
            pltpu.VMEM((BM, BN), bf16),
            pltpu.VMEM((BN, D), f32),
            pltpu.VMEM((BN, D), bf16),
            pltpu.SemaphoreType.DMA((5,)),
        ],
    )


def send_into_job(keep, came):
    def job(place, keep, came, out):
        out[...] = (keep[...] + came[...].astype(f32)).astype(bf16)

    columns = keep.shape[-1]
    half = pl.BlockSpec((None, None, QD, columns), lambda k, p: (k, 1 - p[0], 0, 0))
    return [(keep, half), (came, half)], [(shaped(2, QD, columns), pl.BlockSpec((None, QD, columns), lambda k, p: (k, 0, 0)), None)], job, ()


def send_down_job(keep, came):
    def job(place, keep, came, out):
        out[...] = (keep[...] + came[...].astype(f32)).astype(bf16)

    rows = keep.shape[1]
    theirs = pl.BlockSpec((None, rows // 2, D), lambda k, p: (1, k, 0))
    return [(keep, theirs), (came, theirs)], [(shaped(rows, D), pl.BlockSpec((rows // 2, D), lambda k, p: (k, 0)), None)], job, ()


def back1(place, after, dgu, dy, h, w_gate, w_up, jobs=()):
    WN = 2 * BN

    def body(place, dgu, wg, wu, h, dy, o, acc):
        j = pl.program_id(1)
        for r in cuts(BM, RS):
            for which, w in enumerate((wg, wu)):
                new = lax.dot_general(dgu[which, r, :], w[...], NT, preferred_element_type=f32)
                acc[which, r, :] = added(j == 0, acc[which, r, :], new)

        def last():
            @pl.when(j == F // WN - 1)
            def _():
                def rows_of(r, _):
                    r = pl.ds(pl.multiple_of(r * 256, 256), 256)
                    da = (acc[0, r, :].astype(bf16) + acc[1, r, :].astype(bf16)).astype(f32)
                    wide = h[r, :].astype(f32)
                    scale = lax.rsqrt(jnp.mean(wide * wide, -1, keepdims=True) + 1e-6)
                    along = jnp.mean(da * wide, -1, keepdims=True)
                    dwide = (da * scale - wide * (along * scale * scale * scale)).astype(bf16)
                    o[r, :] = dy[r, :] + dwide
                    return 0

                lax.fori_loop(0, BM // 256, rows_of, 0)

        return last

    into = pl.BlockSpec((None, D, WN), lambda i, j, p: (1, 0, j))
    plain = pl.BlockSpec((BM, D), lambda i, j, p: (i, 0))
    return call(
        body,
        place,
        after,
        [(dgu, pl.BlockSpec((2, BM, WN), lambda i, j, p: (0, i, j))), (w_gate, into), (w_up, into), (h, plain), (dy, plain)],
        [(shaped(T // BM, BM, D), pl.BlockSpec((None, BM, D), lambda i, j, p: (i, 0, 0)), None)],
        (T // BM, F // WN),
        [pltpu.VMEM((2, BM, D), f32)],
        jobs,
    )


def back0(place, after, span, dhs, gate, up, aT, w_down, jobs=()):
    first, _, tiles = span
    steps = TT // BM
    arrays = []
    for array, _ in dhs:
        if not any(array is one for one in arrays):
            arrays.append(array)

    def body(place, *refs):
        refs, (g_r, u_r, aT, wd, into_own, into_out, dgu, total, dh, sem) = refs[: len(arrays)], refs[len(arrays) :]
        j, i = pl.program_id(0), pl.program_id(1)

        def copy(k):
            array, index = dhs[k]
            source = refs[next(n for n, one in enumerate(arrays) if one is array)]
            return pltpu.make_async_copy(source.at[index], dh.at[k], sem.at[k])

        @pl.when((j == 0) & (i == 0))
        def _():
            for k in range(steps):
                copy(k).start()

        for k in range(steps):
            pl.when((j == 0) & (i == k))(lambda k=k: copy(k).wait())

        for r in cuts(BM, RS):
            for c in cuts(BN, CS):
                back = lax.dot_general(dh[i, r, :], wd[c, :], NT, preferred_element_type=f32).astype(bf16).astype(f32)
                _, dgu[0, r, c], dgu[1, r, c] = gated(g_r[r, c], u_r[r, c], back)
        for k in range(2):
            total[k] = added(i == 0, total[k], dot(aT[...], dgu[k]))

        def last():
            @pl.when(i == steps - 1)
            def _():
                into_own[...] = total[:, pl.ds(pl.multiple_of(place[1] * QD, QD), QD), :]
                into_out[...] = total[:, pl.ds(pl.multiple_of((1 - place[1]) * QD, QD), QD), :].astype(bf16)

        return last

    wide = pl.BlockSpec((BM, BN), lambda j, i, p: (i, first + j))
    block = pl.BlockSpec((2, QD, BN), lambda j, i, p: (0, 0, j))
    return call(
        body,
        place,
        after,
        [(array, ANY) for array in arrays]
        + [
            (gate, wide),
            (up, wide),
            (aT, pl.BlockSpec((2 * QD, BM), lambda j, i, p: (p[0], i))),
            (w_down, pl.BlockSpec((None, BN, D), lambda j, i, p: (0, first + j, 0))),
        ],
        [(shaped(2, QD, tiles * BN, dtype=f32), block, None), (shaped(2, QD, tiles * BN), block, None)],
        (tiles, steps),
        [
            pltpu.VMEM((2, BM, BN), bf16),
            pltpu.VMEM((2, 2 * QD, BN), f32),
            pltpu.VMEM((steps, BM, D), bf16),
            pltpu.SemaphoreType.DMA((steps,)),
        ],
        jobs,
    )


def grad_down(place, after, hidden, dhs):
    rows = 384
    n = QF // rows

    def tile(i, place):
        return jnp.where(i < n, place[1] * n + i, (1 - place[1]) * n + i - n)

    def body(place, hidden, *refs):
        dhs, (own, out) = refs[:-2], refs[-2:]
        i = pl.program_id(0)
        total = None
        for k, dh in enumerate(dhs):
            term = lax.dot_general(hidden[k * BM : (k + 1) * BM, :], dh[...], TN, preferred_element_type=f32)
            total = term if total is None else total + term

        @pl.when(i < n)
        def _():
            own[...] = total

        @pl.when(i >= n)
        def _():
            out[...] = total.astype(bf16)

    once = pl.Buffered(1)
    return call(
        body,
        place,
        after,
        [(hidden, pl.BlockSpec((TT, rows), lambda i, p: (0, tile(i, p))))]
        + [(b, pl.BlockSpec((None, BM, D), lambda i, p, k=k: (k, 0, 0), pipeline_mode=once)) for b, k in dhs],
        [
            (shaped(QF, D, dtype=f32), pl.BlockSpec((rows, D), lambda i, p: (jnp.minimum(i, n - 1), 0)), None),
            (shaped(QF, D), pl.BlockSpec((rows, D), lambda i, p: (jnp.maximum(i - n, 0), 0)), None),
        ],
        (2 * n,),
    )


def adamw(g, w, m, v):
    g = g.astype(bf16).astype(f32)
    m = 0.9 * m + 0.1 * g
    v = 0.95 * v + 0.05 * g * g
    return (w - 0.02 * (m * lax.rsqrt(v + 1e-8) + 0.1 * w)).astype(bf16), m, v


def nothing(place):
    pass


def down_job(layer, chunks, own, came, far, w, m, v, held):
    on0, on1, n = chunks

    def job(place, *refs):
        terms, (w, m, v, new_o, m_o, v_o) = refs[:-6], refs[-6:]
        g = sum(term[...].astype(f32) for term in terms)
        new_o[...], m_o[...], v_o[...] = adamw(g, w[...].astype(f32), m[...], v[...])

    def at(s, p):
        return s + jnp.where(p[1] == 0, on0, on1)

    block = pl.BlockSpec((NQ, D), lambda s, p: (s, 0))
    ours = pl.BlockSpec((None, NQ, D), lambda s, p: (0, s, 0)) if far else block
    kept = pl.BlockSpec((None, NQ, D), lambda s, p: (layer, at(s, p), 0))
    whole = pl.BlockSpec((None, NQ, D), lambda s, p: (layer, (2 * p[0] + p[1]) * 3 + at(s, p), 0))
    ins = [(own, ours), (came, ours)] + [(one, block) for one in far] + [(w, whole), (m, kept), (v, kept)]
    outs = [(shaped(n * NQ, D), block, None)]
    outs += [(shaped(2, QF, D, dtype=f32), kept, one) for one in held]
    return ins, outs, job, ()


def into_job(layer, span, parts, ws, ms, vs, held):
    first, stride, tiles = span
    columns = 384
    per = BN // columns
    terms = len(parts)

    def at(s):
        return (first + stride * (s // per)) * per + s % per

    def job(place, *refs):
        parts, refs = refs[:terms], refs[terms:]
        ws, ms, vs = refs[:2], refs[2:4], refs[4:6]
        new, m_o, v_o = refs[6], refs[7:9], refs[9:11]
        for k in range(2):
            g = sum(part[k].astype(f32) for part in parts)
            new[k], m_o[k][...], v_o[k][...] = adamw(g, ws[k][...].astype(f32), ms[k][...], vs[k][...])

    block = pl.BlockSpec((2, QD, columns), lambda s, p: (0, 0, s))
    of_both = pl.BlockSpec((2, None, QD, columns), lambda s, p: (0, p[0], 0, s))
    whole = pl.BlockSpec((None, QD, columns), lambda s, p: (layer, 2 * p[0] + p[1], at(s)))
    kept = pl.BlockSpec((None, QD, columns), lambda s, p: (layer, 0, at(s)))
    ins = [(part, of_both if part.ndim == 4 else block) for part in parts]
    ins += [(w, whole) for w in ws] + [(m, kept) for m in ms] + [(v, kept) for v in vs]
    outs = [(shaped(2, QD, tiles * BN), block, None)] + [(shaped(2, QD, F, dtype=f32), kept, one) for one in held]
    return ins, outs, job, ()


def alone(place, after, grid, jobs):
    return call(nothing, place, after, [], [], grid, jobs=jobs)


def down_pieces(layer, chunks, blocks):
    on0, on1, n = chunks
    rows = n * NQ // 2
    for r, block in enumerate(blocks):
        for h in range(2):

            def there(place, r=r, h=h):
                d = jnp.bitwise_xor(2 * place[0] + place[1], r)
                at = d * QF + jnp.where(lax.rem(d, 2) == 0, on0, on1) * NQ + h * rows
                return layer, pl.ds(pl.multiple_of(at, 192), rows), slice(None)

            yield block, (slice(h * rows, (h + 1) * rows), slice(None)), "down", there


def into_pieces(layer, span, blocks):
    first, stride, tiles = span
    if stride == 1:
        places = [(0, first, tiles)]
    else:
        places = [(j, first + stride * j, 1) for j in range(tiles)]
    for r, block in enumerate(blocks):
        for k, name in enumerate(("gate", "up")):
            for here, to, n in places:

                def there(place, r=r, to=to, n=n):
                    d = jnp.bitwise_xor(2 * place[0] + place[1], r)
                    return layer, pl.ds(pl.multiple_of(d * QD, QD), QD), slice(to * BN, (to + n) * BN)

                yield block, (k, slice(None), slice(here * BN, (here + n) * BN)), name, there


def copy_job(grid, q, pieces, held):
    pieces = list(pieces)
    sources, names = [], []
    for block, _, name, _ in pieces:
        if not any(block is one for one in sources):
            sources.append(block)
        if name not in names:
            names.append(name)
    block, part, _, _ = pieces[0]
    shape = jax.eval_shape(lambda b: b[part], block).shape
    groups = [pieces[at : at + q] for at in range(0, len(pieces), q)]
    steps = grid[0] * (grid[1] if len(grid) > 1 else 1)
    assert steps >= len(groups) + 2

    def body(place, *refs):
        outs, (buffer, reads, writes) = dict(zip(names, refs[len(sources) : -3], strict=True)), refs[-3:]
        step = pl.program_id(0) if len(grid) == 1 else pl.program_id(0) * grid[1] + pl.program_id(1)

        def copies(g):
            for n, (block, part, name, there) in enumerate(groups[g]):
                source = refs[next(k for k, one in enumerate(sources) if one is block)]
                slot = (g % 2) * q + n
                yield (
                    functools.partial(pltpu.make_async_copy, source.at[part], buffer.at[slot], reads.at[slot]),
                    functools.partial(pltpu.make_async_copy, buffer.at[slot], outs[name].at[there(place)], writes.at[slot]),
                )

        for s in range(len(groups) + 2):

            @pl.when(step == s)
            def _(s=s):
                if s >= 2:
                    for _, write in copies(s - 2):
                        write().wait()
                if s < len(groups):
                    for read, _ in copies(s):
                        read().start()
                if 1 <= s <= len(groups):
                    for read, write in copies(s - 1):
                        read().wait()
                        write().start()

    body.copies = True
    whole = {"gate": shaped(2, D, F), "up": shaped(2, D, F), "down": shaped(2, F, D)}
    outs = [(whole[name], ANY, held[name]) for name in names]
    scratch = (pltpu.VMEM((2 * q,) + shape, bf16), pltpu.SemaphoreType.DMA((2 * q,)), pltpu.SemaphoreType.DMA((2 * q,)))
    return [(one, ANY) for one in sources], outs, body, scratch


def spread(new):
    far = over(new, OVER_X)
    near = over(new, OVER_CORE)
    return [new, near, far, over(far, OVER_CORE)]


def whole_step(x, dy, w_gate, w_up, w_down, m_gate, m_up, m_down, v_gate, v_up, v_down):
    d = lax.axis_index("dp")
    place = jnp.stack([d // 2, d % 2]).astype(jnp.int32)
    x, dy = x[0], dy[0]
    x_far = over(x, OVER_X)

    weights = (w_gate, w_up, w_down)
    (gate, up, hid0, aT0, h, a1, aT1), t = forward0(place, None, 0, x, *weights, [None] * 4, True)

    mv = {"into": (None,) * 4, "down": (None,) * 2}
    ALL, ONE, TWO = (0, 0, 3), (2, 0, 1), (0, 1, 2)

    def into(layer, span, *parts):
        return into_job(layer, span, parts, (w_gate, w_up), (m_gate, m_up), (v_gate, v_up), mv["into"])

    def down(layer, chunks, own, came, *far):
        return down_job(layer, chunks, own, came, far, w_down, m_down, v_down, mv["down"])

    def took(results, kind):
        new, *mv[kind] = results
        return spread(new)

    dgu = None
    terms, new1 = {}, {}

    SPANS = {"p": (1, 1, 1), "q": (4, 1, 1), "r": (0, 3, 1), "s": (3, 3, 1), "t": (2, 3, 2)}

    def gradients(t, name, held_down):
        nonlocal dgu
        (dgu, keep, out, *downs), t = layer1(place, t, SPANS[name], a1, aT1, dy, *weights, [dgu, *held_down])
        terms[name] = [keep, over(out, OVER_CORE)]
        return t, downs

    def send(t, name, downs=None):
        jobs = [send_into_job(*terms[name])]
        if downs is not None:
            downs[1] = over(downs[1], OVER_CORE)
            jobs.append(send_down_job(*downs))
        results, t = call(nothing, place, t, [], [], (2,), jobs=jobs)
        terms[name].append(over(results[0], OVER_X))
        if downs is not None:
            downs.append(over(results[1], OVER_X))
        return t

    def adam(t, name):
        span = SPANS[name]
        results, t = alone(place, t, (2 * span[2],), [into(1, span, *terms[name])])
        new1[name] = took(results, "into")
        return t

    def adam_down(t, chunks, downs):
        results, t = alone(place, t, (chunks[2],), [down(1, chunks, *downs)])
        return took(results, "down"), t

    t, downs1 = gradients(t, "p", (None, None))
    t = send(t, "p")
    t, downs1 = gradients(t, "q", downs1)
    t = adam(t, "p")
    t = send(t, "q", downs1)
    t, downs2 = gradients(t, "r", (None, None))
    t = adam(t, "q")
    t = send(t, "r")
    t, downs2 = gradients(t, "s", downs2)
    down1, t = adam_down(t, ONE, downs1)
    t = send(t, "s")
    t = adam(t, "r")
    t, downs2 = gradients(t, "t", downs2)
    t = send(t, "t", downs2)
    (dh,), t = back1(place, t, dgu, dy, h, w_gate, w_up)
    dh_far = over(dh, OVER_X)
    t = adam(t, "s")
    t = adam(t, "t")
    down2, t = adam_down(t, TWO, downs2)
    (gate, up, hid0, aT0), t = forward0(place, t, T // BM, x_far, *weights, [gate, up, hid0, aT0], False)
    dhs = [(dh, 0), (dh, 1), (dh_far, 0), (dh_far, 1)]

    weights_out = {"gate": None, "up": None, "down": None}

    def copying(grid, q, pieces):
        return copy_job(grid, q, pieces, weights_out)

    def copied(results, names):
        weights_out.update(zip(names, results, strict=True))

    (own_d, out_d), t = grad_down(place, t, hid0, dhs)
    came_d = over(out_d, OVER_CORE)
    results, t = alone(place, t, (3,), [down(0, ALL, own_d, came_d)])
    down0 = took(results, "down")

    def first_pieces(*names):
        return [piece for name in names for piece in into_pieces(1, SPANS[name], new1[name])]

    new0 = {}
    spans = {"a": (0, 1, 3), "c": (3, 1, 2), "d": (5, 1, 1)}
    beside = {
        "a": lambda: [copying((3, 4), 4, first_pieces("p", "q", "r", "s")), copying((3, 4), 1, down_pieces(1, ONE, down1))],
        "c": lambda: [
            copying((2, 4), 4, first_pieces("t")),
            copying((2, 4), 2, [*down_pieces(1, TWO, down2)]),
        ],
        "d": lambda: [copying((1, 4), 4, down_pieces(0, ALL, down0))],
    }
    for name, span in spans.items():
        (own, out, *results), t = back0(place, t, span, dhs, gate, up, aT0, w_down, beside[name]())
        copied(results, ("gate", "up", "down")[-len(results) :])
        came = over(out, OVER_CORE)
        results, t = alone(place, t, (2 * span[2],), [into(0, span, own, came)])
        new0[name] = took(results, "into")

    for name, q in (("a", 4), ("c", 8), ("d", 8)):
        grid = (8 // q + 2,)
        results, t = call(nothing, place, t, [], [], grid, jobs=[copying(grid, q, into_pieces(0, spans[name], new0[name]))])
        copied(results, ("gate", "up"))
    held, o_down = (weights_out["gate"], weights_out["up"]), weights_out["down"]
    (m_gate, m_up, v_gate, v_up), (m_down, v_down) = mv["into"], mv["down"]
    return *held, o_down, m_gate, m_up, m_down, v_gate, v_up, v_down


def solution(mesh):
    sequences, whole = P(("rep", "dp"), None, None), P(None, None, None)
    block, group, own = P(None, "dp", None), P("rep", None, None), P("rep", "dp", None)
    return jax.shard_map(
        whole_step,
        mesh=mesh,
        in_specs=(sequences,) * 2 + (whole,) * 3 + (block,) * 6,
        out_specs=(group,) * 3 + (own,) * 6,
        check_vma=False,
    )
```

```python
import functools

import jax
import jax.numpy as jnp
from jax import lax
from jax.experimental import pallas as pl
from jax.experimental.pallas import tpu as pltpu
from jax.sharding import PartitionSpec as P


f32, bf16 = jnp.float32, jnp.bfloat16
T, D, F = 2048, 1152, 4608
TT = 2 * T
HALF = F // 2
BM, BN = 1024, 768
NF, NH = F // BN, HALF // BN
RS, CS = 512, 256
NQ = 384
VMEM = 67043328
QD, QF = D // 4, F // 4
ANY = pl.BlockSpec(memory_space=pl.ANY)
TOKEN = jax.ShapeDtypeStruct((8, 128), jnp.int32)
NT = (((1,), (1,)), ((), ()))
TN = (((0,), (0,)), ((), ()))

OVER_X = [(d, d ^ 2) for d in range(4)]
OVER_CORE = [(d, d ^ 1) for d in range(4)]


def over(array, pairs):
    return lax.ppermute(array, "dp", pairs)


def sigmoid(g):
    return 0.5 * jnp.tanh(0.5 * g) + 0.5


def cuts(n, size):
    return [slice(at, at + size) for at in range(0, n, size)]


def added(first, total, new):
    return jnp.where(first, 0.0, total) + new


def gated(g, u, back):
    s = sigmoid(g)
    silu = g * s
    return (silu * u).astype(bf16), (back * u * (s + silu * (1 - s))).astype(bf16), (back * silu).astype(bf16)


def dot(a, b):
    return jnp.dot(a, b, preferred_element_type=f32)


def call(body, place, after, ins, outs, grid, scratch=(), jobs=()):
    bodies = [(body, len(ins), len(outs), len(scratch))] + [(job, len(i), len(o), len(s)) for i, o, job, s in jobs]
    ins = list(ins) + [one for i, _, _, _ in jobs for one in i]
    outs = list(outs) + [one for _, o, _, _ in jobs for one in o]
    scratch = list(scratch) + [one for _, _, _, s in jobs for one in s]
    arrays = [a for a, _ in ins]
    specs = [s for _, s in ins]
    aliases = {}
    held = [(k, buffer) for k, (_, _, buffer) in enumerate(outs) if buffer is not None]
    for n, (k, buffer) in enumerate(held):
        aliases[1 + len(arrays) + n] = k
    arrays += [buffer for _, buffer in held]
    specs += [ANY] * len(held)
    if after is not None:
        arrays.append(after)
        specs.append(ANY)
    skip = len(arrays) - len(ins)

    def kernel(place_ref, *refs):
        refs, rest = refs[: len(ins)], refs[len(ins) + skip :]
        results, token, own = rest[: len(outs)], rest[len(outs)], rest[len(outs) + 1 :]
        token[...] = jnp.zeros_like(token)
        parts = []
        at_in = at_out = at = 0
        for one, n_in, n_out, n in bodies:
            mine = (*refs[at_in : at_in + n_in], *results[at_out : at_out + n_out], *own[at : at + n])
            parts.append(functools.partial(one, place_ref, *mine))
            at_in, at_out, at = at_in + n_in, at_out + n_out, at + n
        for part, (one, *_) in zip(parts, bodies, strict=True):
            if getattr(one, "copies", False):
                part()
        last = [part() for part, (one, *_) in zip(parts, bodies, strict=True) if not getattr(one, "copies", False)]
        if last[0] is not None:
            last[0]()

    result = pl.pallas_call(
        kernel,
        grid_spec=pltpu.PrefetchScalarGridSpec(
            num_scalar_prefetch=1,
            grid=grid,
            in_specs=specs,
            out_specs=[s for _, s, _ in outs] + [pl.BlockSpec((8, 128), lambda *_: (0, 0))],
            scratch_shapes=scratch,
        ),
        out_shape=[o for o, _, _ in outs] + [TOKEN],
        input_output_aliases=aliases,
        cost_estimate=pl.CostEstimate(flops=T * D * F, bytes_accessed=T * D * F, transcendentals=0),
        compiler_params=pltpu.CompilerParams(vmem_limit_bytes=VMEM),
    )(place, *arrays)
    return result[:-1], result[-1]


def shaped(*shape, dtype=bf16):
    return jax.ShapeDtypeStruct(shape, dtype)


def normalise(h, a_s, aT):
    def rows_of(i, _):
        rows = pl.ds(pl.multiple_of(i * 256, 256), 256)
        wide = h[rows, :].astype(f32)
        scale = lax.rsqrt(jnp.mean(wide * wide, -1, keepdims=True) + 1e-6)
        a = (wide * scale).astype(bf16)
        a_s[rows, :] = a
        if aT is not None:
            aT[:, rows] = a.T
        return 0

    lax.fori_loop(0, h.shape[0] // 256, rows_of, 0)


def forward0(place, after, first, x, w_gate, w_up, w_down, held, whole):
    rows = x.shape[0]

    def tile(j, place):
        return jnp.where(j < NH, place[0] * NH + j, (1 - place[0]) * NH + j - NH)

    def body(place, x, wg, wu, *refs):
        if whole:
            wd, g_o, u_o, hid_o, aT_o, h_o, a1_o, a_s, hs, acc = refs
        else:
            g_o, u_o, hid_o, aT_o, a_s, hs = refs
        j = pl.program_id(1)

        @pl.when(j == 0)
        def _():
            normalise(x, a_s, aT_o)

        for r in cuts(BM, RS):
            a = a_s[r, :]
            for c in cuts(BN, CS):
                g, u = dot(a, wg[:, c]), dot(a, wu[:, c])
                g_o[r, c] = g
                u_o[r, c] = u
                hs[r, c] = (g * sigmoid(g) * u).astype(bf16)
            if whole:
                acc[r, :] = added(j == 0, acc[r, :], dot(hs[r, :], wd[...]))

        @pl.when(j < NH)
        def _():
            hid_o[...] = hs[...]

        if whole:

            @pl.when(j == NF - 1)
            def _():
                def rows_of(i, _):
                    rows = pl.ds(pl.multiple_of(i * 256, 256), 256)
                    h_o[rows, :] = x[rows, :] + acc[rows, :].astype(bf16)
                    return 0

                lax.fori_loop(0, BM // 256, rows_of, 0)
                normalise(h_o, a1_o, None)

    wide = pl.BlockSpec((BM, BN), lambda i, j, p: (first + i, tile(j, p)))
    into = pl.BlockSpec((None, D, BN), lambda i, j, p: (0, 0, tile(j, p)))
    plain = pl.BlockSpec((BM, D), lambda i, j, p: (i, 0))
    ins = [(x, plain), (w_gate, into), (w_up, into)]
    outs = [
        (shaped(TT, F, dtype=f32), wide, held[0]),
        (shaped(TT, F, dtype=f32), wide, held[1]),
        (shaped(TT, HALF), pl.BlockSpec((BM, BN), lambda i, j, p: (first + i, jnp.minimum(j, NH - 1))), held[2]),
        (shaped(D, TT), pl.BlockSpec((D, BM), lambda i, j, p: (0, first + i)), held[3]),
    ]
    scratch = [pltpu.VMEM((BM, D), bf16), pltpu.VMEM((BM, BN), bf16)]
    if whole:
        ins += [(w_down, pl.BlockSpec((None, BN, D), lambda i, j, p: (0, tile(j, p), 0)))]
        outs += [(shaped(T, D), plain, None), (shaped(T, D), plain, None)]
        scratch += [pltpu.VMEM((BM, D), f32)]
    return call(body, place, after, ins, outs, (rows // BM, NF), scratch)


def layer1(place, after, span, a1, dy, w_gate, w_up, w_down, held):
    steps = T // BM
    first, stride, tiles = span
    t = first % NH
    rows = NQ if t == 1 else 2 * NQ

    def at(j):
        return first + stride * j

    def body(place, a1, dy, wg, wu, wd, dgu_o, keep, out, down_keep, down_out, total, leaving, hid, down, down_leaving, sem):
        j, i = pl.program_id(0), pl.program_id(1)
        core = place[1]

        def mine(x, core):
            return pl.ds(pl.multiple_of((2 * x + core) * QD, QD), QD)

        def each(j, act):
            side = jnp.where(place[0] == at(j) // NH, 0, 1)
            columns = pl.ds(pl.multiple_of(j * BN, BN), BN)
            for x in range(2):
                act(pltpu.make_async_copy(total.at[:, mine(x, core), :], keep.at[:, x, :, columns], sem.at[x]))
            act(pltpu.make_async_copy(leaving, out.at[:, :, :, columns], sem.at[2]))
            for s in range(2):
                owner = (2 * t + s) // 3
                here, to = pl.ds(s * NQ, NQ), pl.ds(0 if t == 1 else s * NQ, NQ)

                @pl.when(core == owner)
                def _():
                    act(pltpu.make_async_copy(down.at[here, :], down_keep.at[side, to, :], sem.at[3 + s]))

                @pl.when(core != owner)
                def _():
                    act(pltpu.make_async_copy(down_leaving.at[here, :], down_out.at[side, to, :], sem.at[3 + s]))

        @pl.when((j > 0) & (i == 0))
        def _():
            each(j - 1, lambda copy: copy.wait())

        for r in cuts(BM, RS):
            a = a1[r, :]
            for c in cuts(BN, CS):
                g, u = dot(a, wg[:, c]), dot(a, wu[:, c])
                back = lax.dot_general(dy[r, :], wd[c, :], NT, preferred_element_type=f32).astype(bf16).astype(f32)
                hid[r, c], dgu_o[0, r, c], dgu_o[1, r, c] = gated(g, u, back)
        for k in range(2):
            total[k] = added(i == 0, total[k], lax.dot_general(a1[...], dgu_o[k], TN, preferred_element_type=f32))
        down[...] = added(i == 0, down[...], lax.dot_general(hid[...], dy[...], TN, preferred_element_type=f32))

        def last():
            @pl.when(i == steps - 1)
            def _():
                for x in range(2):
                    leaving[:, x] = total[:, mine(x, 1 - core), :].astype(bf16)
                down_leaving[...] = down[...].astype(bf16)
                each(j, lambda copy: copy.start())

            @pl.when((j == tiles - 1) & (i == steps - 1))
            def _():
                each(j, lambda copy: copy.wait())

        return last

    into = pl.BlockSpec((None, D, BN), lambda j, i, p: (1, 0, at(j)))
    plain = pl.BlockSpec((BM, D), lambda j, i, p: (i, 0))
    return call(
        body,
        place,
        after,
        [
            (a1, plain),
            (dy, plain),
            (w_gate, into),
            (w_up, into),
            (w_down, pl.BlockSpec((None, BN, D), lambda j, i, p: (1, at(j), 0))),
        ],
        [
            (shaped(2, T, F), pl.BlockSpec((2, BM, BN), lambda j, i, p: (0, i, at(j))), held[0]),
            (shaped(2, 2, QD, tiles * BN, dtype=f32), ANY, None),
            (shaped(2, 2, QD, tiles * BN), ANY, None),
            (shaped(2, rows, D, dtype=f32), ANY, held[1]),
            (shaped(2, rows, D), ANY, held[2]),
        ],
        (tiles, steps),
        [
            pltpu.VMEM((2, D, BN), f32),
            pltpu.VMEM((2, 2, QD, BN), bf16),
            pltpu.VMEM((BM, BN), bf16),
            pltpu.VMEM((BN, D), f32),
            pltpu.VMEM((BN, D), bf16),
            pltpu.SemaphoreType.DMA((5,)),
        ],
    )


def send_into_job(keep, came):
    def job(place, keep, came, out):
        out[...] = (keep[...] + came[...].astype(f32)).astype(bf16)

    columns = keep.shape[-1]
    half = pl.BlockSpec((None, None, QD, columns), lambda k, p: (k, 1 - p[0], 0, 0))
    return [(keep, half), (came, half)], [(shaped(2, QD, columns), pl.BlockSpec((None, QD, columns), lambda k, p: (k, 0, 0)), None)], job, ()


def send_down_job(keep, came):
    def job(place, keep, came, out):
        out[...] = (keep[...] + came[...].astype(f32)).astype(bf16)

    rows = keep.shape[1]
    theirs = pl.BlockSpec((None, rows // 2, D), lambda k, p: (1, k, 0))
    return [(keep, theirs), (came, theirs)], [(shaped(rows, D), pl.BlockSpec((rows // 2, D), lambda k, p: (k, 0)), None)], job, ()


def back1(place, after, tile, dgu, dy, h, w_gate, w_up):
    WN = 2 * BN

    def body(place, dgu, wg, wu, h, dy, o, acc):
        j = pl.program_id(0)
        for r in cuts(BM, RS):
            for which, w in enumerate((wg, wu)):
                new = lax.dot_general(dgu[which, r, :], w[...], NT, preferred_element_type=f32)
                acc[which, r, :] = added(j == 0, acc[which, r, :], new)

        def last():
            @pl.when(j == F // WN - 1)
            def _():
                def rows_of(r, _):
                    r = pl.ds(pl.multiple_of(r * 256, 256), 256)
                    da = (acc[0, r, :].astype(bf16) + acc[1, r, :].astype(bf16)).astype(f32)
                    wide = h[r, :].astype(f32)
                    scale = lax.rsqrt(jnp.mean(wide * wide, -1, keepdims=True) + 1e-6)
                    along = jnp.mean(da * wide, -1, keepdims=True)
                    dwide = (da * scale - wide * (along * scale * scale * scale)).astype(bf16)
                    o[r, :] = dy[r, :] + dwide
                    return 0

                lax.fori_loop(0, BM // 256, rows_of, 0)

        return last

    into = pl.BlockSpec((None, D, WN), lambda j, p: (1, 0, j))
    plain = pl.BlockSpec((BM, D), lambda j, p: (tile, 0))
    return call(
        body,
        place,
        after,
        [(dgu, pl.BlockSpec((2, BM, WN), lambda j, p: (0, tile, j))), (w_gate, into), (w_up, into), (h, plain), (dy, plain)],
        [(shaped(BM, D), pl.BlockSpec((BM, D), lambda j, p: (0, 0)), None)],
        (F // WN,),
        [pltpu.VMEM((2, BM, D), f32)],
    )


def back0(place, after, span, dhs, gate, up, aT, w_down, jobs=()):
    first, _, tiles = span
    steps = TT // BM

    def body(place, *refs):
        refs, (g_r, u_r, aT, wd, into_own, into_out, dgu, total, dh, sem) = refs[:steps], refs[steps:]
        j, i = pl.program_id(0), pl.program_id(1)

        def copy(k):
            return pltpu.make_async_copy(refs[k], dh.at[k], sem.at[k])

        @pl.when((j == 0) & (i == 0))
        def _():
            for k in range(steps):
                copy(k).start()

        for k in range(steps):
            pl.when((j == 0) & (i == k))(lambda k=k: copy(k).wait())

        for r in cuts(BM, RS):
            for c in cuts(BN, CS):
                back = lax.dot_general(dh[i, r, :], wd[c, :], NT, preferred_element_type=f32).astype(bf16).astype(f32)
                _, dgu[0, r, c], dgu[1, r, c] = gated(g_r[r, c], u_r[r, c], back)
        for k in range(2):
            total[k] = added(i == 0, total[k], dot(aT[...], dgu[k]))

        def last():
            @pl.when(i == steps - 1)
            def _():
                into_own[...] = total[:, pl.ds(pl.multiple_of(place[1] * QD, QD), QD), :]
                into_out[...] = total[:, pl.ds(pl.multiple_of((1 - place[1]) * QD, QD), QD), :].astype(bf16)

        return last

    wide = pl.BlockSpec((BM, BN), lambda j, i, p: (i, first + j))
    block = pl.BlockSpec((2, QD, BN), lambda j, i, p: (0, 0, j))
    return call(
        body,
        place,
        after,
        [(one, ANY) for one in dhs]
        + [
            (gate, wide),
            (up, wide),
            (aT, pl.BlockSpec((2 * QD, BM), lambda j, i, p: (p[0], i))),
            (w_down, pl.BlockSpec((None, BN, D), lambda j, i, p: (0, first + j, 0))),
        ],
        [(shaped(2, QD, tiles * BN, dtype=f32), block, None), (shaped(2, QD, tiles * BN), block, None)],
        (tiles, steps),
        [
            pltpu.VMEM((2, BM, BN), bf16),
            pltpu.VMEM((2, 2 * QD, BN), f32),
            pltpu.VMEM((steps, BM, D), bf16),
            pltpu.SemaphoreType.DMA((steps,)),
        ],
        jobs,
    )


def grad_down(place, after, hidden, dhs):
    rows = 384
    n = QF // rows

    def tile(i, place):
        return jnp.where(i < n, place[1] * n + i, (1 - place[1]) * n + i - n)

    def body(place, hidden, *refs):
        dhs, (own, out) = refs[:-2], refs[-2:]
        i = pl.program_id(0)
        total = None
        for k, dh in enumerate(dhs):
            term = lax.dot_general(hidden[k * BM : (k + 1) * BM, :], dh[...], TN, preferred_element_type=f32)
            total = term if total is None else total + term

        @pl.when(i < n)
        def _():
            own[...] = total

        @pl.when(i >= n)
        def _():
            out[...] = total.astype(bf16)

    once = pl.Buffered(1)
    return call(
        body,
        place,
        after,
        [(hidden, pl.BlockSpec((TT, rows), lambda i, p: (0, tile(i, p))))]
        + [(one, pl.BlockSpec((BM, D), lambda i, p: (0, 0), pipeline_mode=once)) for one in dhs],
        [
            (shaped(QF, D, dtype=f32), pl.BlockSpec((rows, D), lambda i, p: (jnp.minimum(i, n - 1), 0)), None),
            (shaped(QF, D), pl.BlockSpec((rows, D), lambda i, p: (jnp.maximum(i - n, 0), 0)), None),
        ],
        (2 * n,),
    )


def adamw(g, w, m, v):
    g = g.astype(bf16).astype(f32)
    m = 0.9 * m + 0.1 * g
    v = 0.95 * v + 0.05 * g * g
    return (w - 0.02 * (m * lax.rsqrt(v + 1e-8) + 0.1 * w)).astype(bf16), m, v


def nothing(place):
    pass


def down_job(layer, chunks, own, came, far, w, m, v, held):
    on0, on1, n = chunks

    def job(place, *refs):
        terms, (w, m, v, new_o, m_o, v_o) = refs[:-6], refs[-6:]
        g = sum(term[...].astype(f32) for term in terms)
        new_o[...], m_o[...], v_o[...] = adamw(g, w[...].astype(f32), m[...], v[...])

    def at(s, p):
        return s + jnp.where(p[1] == 0, on0, on1)

    block = pl.BlockSpec((NQ, D), lambda s, p: (s, 0))
    ours = pl.BlockSpec((None, NQ, D), lambda s, p: (0, s, 0)) if far else block
    kept = pl.BlockSpec((None, NQ, D), lambda s, p: (layer, at(s, p), 0))
    whole = pl.BlockSpec((None, NQ, D), lambda s, p: (layer, (2 * p[0] + p[1]) * 3 + at(s, p), 0))
    ins = [(own, ours), (came, ours)] + [(one, block) for one in far] + [(w, whole), (m, kept), (v, kept)]
    outs = [(shaped(n * NQ, D), block, None)]
    outs += [(shaped(2, QF, D, dtype=f32), kept, one) for one in held]
    return ins, outs, job, ()


def into_job(layer, span, parts, ws, ms, vs, held):
    first, stride, tiles = span
    columns = 384
    per = BN // columns
    terms = len(parts)

    def at(s):
        return (first + stride * (s // per)) * per + s % per

    def job(place, *refs):
        parts, refs = refs[:terms], refs[terms:]
        ws, ms, vs = refs[:2], refs[2:4], refs[4:6]
        new, m_o, v_o = refs[6], refs[7:9], refs[9:11]
        for k in range(2):
            g = sum(part[k].astype(f32) for part in parts)
            new[k], m_o[k][...], v_o[k][...] = adamw(g, ws[k][...].astype(f32), ms[k][...], vs[k][...])

    block = pl.BlockSpec((2, QD, columns), lambda s, p: (0, 0, s))
    of_both = pl.BlockSpec((2, None, QD, columns), lambda s, p: (0, p[0], 0, s))
    whole = pl.BlockSpec((None, QD, columns), lambda s, p: (layer, 2 * p[0] + p[1], at(s)))
    kept = pl.BlockSpec((None, QD, columns), lambda s, p: (layer, 0, at(s)))
    ins = [(part, of_both if part.ndim == 4 else block) for part in parts]
    ins += [(w, whole) for w in ws] + [(m, kept) for m in ms] + [(v, kept) for v in vs]
    outs = [(shaped(2, QD, tiles * BN), block, None)] + [(shaped(2, QD, F, dtype=f32), kept, one) for one in held]
    return ins, outs, job, ()


def alone(place, after, grid, jobs):
    return call(nothing, place, after, [], [], grid, jobs=jobs)


def down_pieces(layer, chunks, blocks):
    on0, on1, n = chunks
    rows = n * NQ // 2
    for r, block in enumerate(blocks):
        for h in range(2):

            def there(place, r=r, h=h):
                d = jnp.bitwise_xor(2 * place[0] + place[1], r)
                at = d * QF + jnp.where(lax.rem(d, 2) == 0, on0, on1) * NQ + h * rows
                return layer, pl.ds(pl.multiple_of(at, 192), rows), slice(None)

            yield block, (slice(h * rows, (h + 1) * rows), slice(None)), "down", there


def into_pieces(layer, span, blocks):
    first, stride, tiles = span
    if stride == 1:
        places = [(0, first, tiles)]
    else:
        places = [(j, first + stride * j, 1) for j in range(tiles)]
    for r, block in enumerate(blocks):
        for k, name in enumerate(("gate", "up")):
            for here, to, n in places:

                def there(place, r=r, to=to, n=n):
                    d = jnp.bitwise_xor(2 * place[0] + place[1], r)
                    return layer, pl.ds(pl.multiple_of(d * QD, QD), QD), slice(to * BN, (to + n) * BN)

                yield block, (k, slice(None), slice(here * BN, (here + n) * BN)), name, there


def copy_job(grid, q, pieces, held):
    pieces = list(pieces)
    sources, names = [], []
    for block, _, name, _ in pieces:
        if not any(block is one for one in sources):
            sources.append(block)
        if name not in names:
            names.append(name)
    block, part, _, _ = pieces[0]
    shape = jax.eval_shape(lambda b: b[part], block).shape
    groups = [pieces[at : at + q] for at in range(0, len(pieces), q)]
    steps = grid[0] * (grid[1] if len(grid) > 1 else 1)
    assert steps >= len(groups) + 2

    def body(place, *refs):
        outs, (buffer, reads, writes) = dict(zip(names, refs[len(sources) : -3], strict=True)), refs[-3:]
        step = pl.program_id(0) if len(grid) == 1 else pl.program_id(0) * grid[1] + pl.program_id(1)

        def copies(g):
            for n, (block, part, name, there) in enumerate(groups[g]):
                source = refs[next(k for k, one in enumerate(sources) if one is block)]
                slot = (g % 2) * q + n
                yield (
                    functools.partial(pltpu.make_async_copy, source.at[part], buffer.at[slot], reads.at[slot]),
                    functools.partial(pltpu.make_async_copy, buffer.at[slot], outs[name].at[there(place)], writes.at[slot]),
                )

        for s in range(len(groups) + 2):

            @pl.when(step == s)
            def _(s=s):
                if s >= 2:
                    for _, write in copies(s - 2):
                        write().wait()
                if s < len(groups):
                    for read, _ in copies(s):
                        read().start()
                if 1 <= s <= len(groups):
                    for read, write in copies(s - 1):
                        read().wait()
                        write().start()

    body.copies = True
    whole = {"gate": shaped(2, D, F), "up": shaped(2, D, F), "down": shaped(2, F, D)}
    outs = [(whole[name], ANY, held[name]) for name in names]
    scratch = (pltpu.VMEM((2 * q,) + shape, bf16), pltpu.SemaphoreType.DMA((2 * q,)), pltpu.SemaphoreType.DMA((2 * q,)))
    return [(one, ANY) for one in sources], outs, body, scratch


def spread(new):
    far = over(new, OVER_X)
    near = over(new, OVER_CORE)
    return [new, near, far, over(far, OVER_CORE)]


def whole_step(x, dy, w_gate, w_up, w_down, m_gate, m_up, m_down, v_gate, v_up, v_down):
    d = lax.axis_index("dp")
    place = jnp.stack([d // 2, d % 2]).astype(jnp.int32)
    x, dy = x[0], dy[0]
    x_far = over(x, OVER_X)

    weights = (w_gate, w_up, w_down)
    (gate, up, hid0, aT0, h, a1), t = forward0(place, None, 0, x, *weights, [None] * 4, True)

    mv = {"into": (None,) * 4, "down": (None,) * 2}
    ALL, ONE, TWO = (0, 0, 3), (2, 0, 1), (0, 1, 2)

    def into(layer, span, *parts):
        return into_job(layer, span, parts, (w_gate, w_up), (m_gate, m_up), (v_gate, v_up), mv["into"])

    def down(layer, chunks, own, came, *far):
        return down_job(layer, chunks, own, came, far, w_down, m_down, v_down, mv["down"])

    def took(results, kind):
        new, *mv[kind] = results
        return spread(new)

    dgu = None
    terms, new1 = {}, {}

    SPANS = {"p": (1, 1, 1), "q": (4, 1, 1), "r": (0, 3, 1), "s": (3, 3, 1), "u": (2, 3, 1), "v": (5, 3, 1)}

    def gradients(t, name, held_down):
        nonlocal dgu
        (dgu, keep, out, *downs), t = layer1(place, t, SPANS[name], a1, dy, *weights, [dgu, *held_down])
        terms[name] = [keep, over(out, OVER_CORE)]
        return t, downs

    def send(t, name, downs=None):
        jobs = [send_into_job(*terms[name])]
        if downs is not None:
            downs[1] = over(downs[1], OVER_CORE)
            jobs.append(send_down_job(*downs))
        results, t = call(nothing, place, t, [], [], (2,), jobs=jobs)
        terms[name].append(over(results[0], OVER_X))
        if downs is not None:
            downs.append(over(results[1], OVER_X))
        return t

    def adam(t, name):
        span = SPANS[name]
        results, t = alone(place, t, (2 * span[2],), [into(1, span, *terms[name])])
        new1[name] = took(results, "into")
        return t

    def adam_down(t, chunks, downs):
        results, t = alone(place, t, (chunks[2],), [down(1, chunks, *downs)])
        return took(results, "down"), t

    t, downs1 = gradients(t, "p", (None, None))
    t = send(t, "p")
    t, downs1 = gradients(t, "q", downs1)
    t = adam(t, "p")
    t = send(t, "q", downs1)
    t, downs2 = gradients(t, "r", (None, None))
    t = adam(t, "q")
    t = send(t, "r")
    t, downs2 = gradients(t, "s", downs2)
    down1, t = adam_down(t, ONE, downs1)
    t = send(t, "s")
    t = adam(t, "r")
    t, downs2 = gradients(t, "u", downs2)
    t = adam(t, "s")
    t = send(t, "u")
    t, downs2 = gradients(t, "v", downs2)
    t = adam(t, "u")
    t = send(t, "v", downs2)
    dhs, dhs_far = [], []
    for tile in range(T // BM):
        (dh,), t = back1(place, t, tile, dgu, dy, h, w_gate, w_up)
        dhs.append(dh)
        dhs_far.append(over(dh, OVER_X))
    dhs += dhs_far
    t = adam(t, "v")
    (gate, up, hid0, aT0), t = forward0(place, t, T // BM, x_far, *weights, [gate, up, hid0, aT0], False)

    weights_out = {"gate": None, "up": None, "down": None}

    def copying(grid, q, pieces):
        return copy_job(grid, q, pieces, weights_out)

    def copied(results, names):
        weights_out.update(zip(names, results, strict=True))

    (own_d, out_d), t = grad_down(place, t, hid0, dhs)
    came_d = over(out_d, OVER_CORE)
    down2, t = adam_down(t, TWO, downs2)
    results, t = alone(place, t, (3,), [down(0, ALL, own_d, came_d)])
    down0 = took(results, "down")

    def first_pieces(*names):
        return [piece for name in names for piece in into_pieces(1, SPANS[name], new1[name])]

    new0 = {}
    spans = {"a": (0, 1, 3), "c": (3, 1, 2), "d": (5, 1, 1)}
    beside = {
        "a": lambda: [copying((3, 4), 3, first_pieces("p", "q", "r")), copying((3, 4), 1, down_pieces(1, ONE, down1))],
        "c": lambda: [copying((2, 4), 4, first_pieces("s", "u", "v")), copying((2, 4), 2, down_pieces(1, TWO, down2))],
        "d": lambda: [copying((1, 4), 4, down_pieces(0, ALL, down0))],
    }
    for name, span in spans.items():
        (own, out, *results), t = back0(place, t, span, dhs, gate, up, aT0, w_down, beside[name]())
        copied(results, ("gate", "up", "down")[: len(results)] if name != "d" else ("down",))
        came = over(out, OVER_CORE)
        results, t = alone(place, t, (2 * span[2],), [into(0, span, own, came)])
        new0[name] = took(results, "into")

    for name, q in (("a", 4), ("c", 8), ("d", 8)):
        grid = (8 // q + 2,)
        jobs = [copying(grid, q, into_pieces(0, spans[name], new0[name]))]
        results, t = call(nothing, place, t, [], [], grid, jobs=jobs)
        copied(results, ("gate", "up", "down")[: len(results)])
    held, o_down = (weights_out["gate"], weights_out["up"]), weights_out["down"]
    (m_gate, m_up, v_gate, v_up), (m_down, v_down) = mv["into"], mv["down"]
    return *held, o_down, m_gate, m_up, m_down, v_gate, v_up, v_down


def solution(mesh):
    sequences, whole = P(("rep", "dp"), None, None), P(None, None, None)
    block, group, own = P(None, "dp", None), P("rep", None, None), P("rep", "dp", None)
    return jax.shard_map(
        whole_step,
        mesh=mesh,
        in_specs=(sequences,) * 2 + (whole,) * 3 + (block,) * 6,
        out_specs=(group,) * 3 + (own,) * 6,
        check_vma=False,
    )
```

```python
import functools

import jax
import jax.numpy as jnp
from jax import lax
from jax.experimental import pallas as pl
from jax.experimental.pallas import tpu as pltpu
from jax.sharding import PartitionSpec as P


f32, bf16 = jnp.float32, jnp.bfloat16
T, D, F = 2048, 1152, 4608
TT = 2 * T
HALF = F // 2
BM, BN = 1024, 768
NF, NH = F // BN, HALF // BN
RS, CS = 512, 256
NQ = 384
VMEM = 67043328
QD, QF = D // 4, F // 4
ANY = pl.BlockSpec(memory_space=pl.ANY)
TOKEN = jax.ShapeDtypeStruct((8, 128), jnp.int32)
NT = (((1,), (1,)), ((), ()))
TN = (((0,), (0,)), ((), ()))

OVER_X = [(d, d ^ 2) for d in range(4)]
OVER_CORE = [(d, d ^ 1) for d in range(4)]


def over(array, pairs):
    return lax.ppermute(array, "dp", pairs)


def sigmoid(g):
    return 0.5 * jnp.tanh(0.5 * g) + 0.5


def cuts(n, size):
    return [slice(at, at + size) for at in range(0, n, size)]


def added(first, total, new):
    return jnp.where(first, 0.0, total) + new


def gated(g, u, back):
    s = sigmoid(g)
    silu = g * s
    return (silu * u).astype(bf16), (back * u * (s + silu * (1 - s))).astype(bf16), (back * silu).astype(bf16)


def dot(a, b):
    return jnp.dot(a, b, preferred_element_type=f32)


def call(body, place, after, ins, outs, grid, scratch=(), jobs=()):
    bodies = [(body, len(ins), len(outs), len(scratch))] + [(job, len(i), len(o), len(s)) for i, o, job, s in jobs]
    ins = list(ins) + [one for i, _, _, _ in jobs for one in i]
    outs = list(outs) + [one for _, o, _, _ in jobs for one in o]
    scratch = list(scratch) + [one for _, _, _, s in jobs for one in s]
    arrays = [a for a, _ in ins]
    specs = [s for _, s in ins]
    aliases = {}
    held = [(k, buffer) for k, (_, _, buffer) in enumerate(outs) if buffer is not None]
    for n, (k, buffer) in enumerate(held):
        aliases[1 + len(arrays) + n] = k
    arrays += [buffer for _, buffer in held]
    specs += [ANY] * len(held)
    if after is not None:
        arrays.append(after)
        specs.append(ANY)
    skip = len(arrays) - len(ins)

    def kernel(place_ref, *refs):
        refs, rest = refs[: len(ins)], refs[len(ins) + skip :]
        results, token, own = rest[: len(outs)], rest[len(outs)], rest[len(outs) + 1 :]
        token[...] = jnp.zeros_like(token)
        parts = []
        at_in = at_out = at = 0
        for one, n_in, n_out, n in bodies:
            mine = (*refs[at_in : at_in + n_in], *results[at_out : at_out + n_out], *own[at : at + n])
            parts.append(functools.partial(one, place_ref, *mine))
            at_in, at_out, at = at_in + n_in, at_out + n_out, at + n
        for part, (one, *_) in zip(parts, bodies, strict=True):
            if getattr(one, "copies", False):
                part()
        last = [part() for part, (one, *_) in zip(parts, bodies, strict=True) if not getattr(one, "copies", False)]
        if last[0] is not None:
            last[0]()

    result = pl.pallas_call(
        kernel,
        grid_spec=pltpu.PrefetchScalarGridSpec(
            num_scalar_prefetch=1,
            grid=grid,
            in_specs=specs,
            out_specs=[s for _, s, _ in outs] + [pl.BlockSpec((8, 128), lambda *_: (0, 0))],
            scratch_shapes=scratch,
        ),
        out_shape=[o for o, _, _ in outs] + [TOKEN],
        input_output_aliases=aliases,
        cost_estimate=pl.CostEstimate(flops=T * D * F, bytes_accessed=T * D * F, transcendentals=0),
        compiler_params=pltpu.CompilerParams(vmem_limit_bytes=VMEM),
    )(place, *arrays)
    return result[:-1], result[-1]


def shaped(*shape, dtype=bf16):
    return jax.ShapeDtypeStruct(shape, dtype)


def normalise(h, a):
    def rows_of(i, _):
        rows = pl.ds(pl.multiple_of(i * 256, 256), 256)
        wide = h[rows, :].astype(f32)
        scale = lax.rsqrt(jnp.mean(wide * wide, -1, keepdims=True) + 1e-6)
        a[rows, :] = (wide * scale).astype(bf16)
        return 0

    lax.fori_loop(0, h.shape[0] // 256, rows_of, 0)


def forward0(place, after, first, x, w_gate, w_up, w_down, held, whole):
    rows = x.shape[0]

    def tile(j, place):
        return jnp.where(j < NH, place[0] * NH + j, (1 - place[0]) * NH + j - NH)

    def body(place, x, wg, wu, *refs):
        if whole:
            wd, g_o, u_o, hid_o, aT_o, h_o, a1_o, a_s, hs, acc = refs
        else:
            g_o, u_o, hid_o, aT_o, a_s, hs = refs
        j = pl.program_id(1)

        @pl.when(j == 0)
        def _():
            normalise(x, a_s)

        part = pl.ds(pl.multiple_of(jnp.minimum(j * 256, BM - 256), 256), 256)
        aT_o[:, part] = a_s[part, :].T
        for r in cuts(BM, RS):
            a = a_s[r, :]
            for c in cuts(BN, CS):
                g, u = dot(a, wg[:, c]), dot(a, wu[:, c])
                g_o[r, c] = g
                u_o[r, c] = u
                hs[r, c] = (g * sigmoid(g) * u).astype(bf16)
            if whole:
                acc[r, :] = added(j == 0, acc[r, :], dot(hs[r, :], wd[...]))

        @pl.when(j < NH)
        def _():
            hid_o[...] = hs[...]

        if whole:

            @pl.when(j == NF - 1)
            def _():
                def rows_of(i, _):
                    rows = pl.ds(pl.multiple_of(i * 256, 256), 256)
                    h_o[rows, :] = x[rows, :] + acc[rows, :].astype(bf16)
                    return 0

                lax.fori_loop(0, BM // 256, rows_of, 0)
                normalise(h_o, a1_o)

    wide = pl.BlockSpec((BM, BN), lambda i, j, p: (first + i, tile(j, p)))
    into = pl.BlockSpec((None, D, BN), lambda i, j, p: (0, 0, tile(j, p)))
    plain = pl.BlockSpec((BM, D), lambda i, j, p: (i, 0))
    ins = [(x, plain), (w_gate, into), (w_up, into)]
    outs = [
        (shaped(TT, F, dtype=f32), wide, held[0]),
        (shaped(TT, F, dtype=f32), wide, held[1]),
        (shaped(TT, HALF), pl.BlockSpec((BM, BN), lambda i, j, p: (first + i, jnp.minimum(j, NH - 1))), held[2]),
        (shaped(D, TT), pl.BlockSpec((D, BM), lambda i, j, p: (0, first + i)), held[3]),
    ]
    scratch = [pltpu.VMEM((BM, D), bf16), pltpu.VMEM((BM, BN), bf16)]
    if whole:
        ins += [(w_down, pl.BlockSpec((None, BN, D), lambda i, j, p: (0, tile(j, p), 0)))]
        outs += [(shaped(T, D), plain, None), (shaped(T, D), plain, None)]
        scratch += [pltpu.VMEM((BM, D), f32)]
    return call(body, place, after, ins, outs, (rows // BM, NF), scratch)


def layer1(place, after, span, a1, dy, w_gate, w_up, w_down, held):
    steps = T // BM
    first, stride, tiles = span
    t = first % NH
    rows = NQ if t == 1 else 2 * NQ

    def at(j):
        return first + stride * j

    def body(place, a1, dy, wg, wu, wd, dgu_o, keep, out, down_keep, down_out, total, leaving, hid, down, down_leaving, sem):
        j, i = pl.program_id(0), pl.program_id(1)
        core = place[1]

        def mine(x, core):
            return pl.ds(pl.multiple_of((2 * x + core) * QD, QD), QD)

        def each(j, act):
            side = jnp.where(place[0] == at(j) // NH, 0, 1)
            columns = pl.ds(pl.multiple_of(j * BN, BN), BN)
            for x in range(2):
                act(pltpu.make_async_copy(total.at[:, mine(x, core), :], keep.at[:, x, :, columns], sem.at[x]))
            act(pltpu.make_async_copy(leaving, out.at[:, :, :, columns], sem.at[2]))
            for s in range(2):
                owner = (2 * t + s) // 3
                here, to = pl.ds(s * NQ, NQ), pl.ds(0 if t == 1 else s * NQ, NQ)

                @pl.when(core == owner)
                def _():
                    act(pltpu.make_async_copy(down.at[here, :], down_keep.at[side, to, :], sem.at[3 + s]))

                @pl.when(core != owner)
                def _():
                    act(pltpu.make_async_copy(down_leaving.at[here, :], down_out.at[side, to, :], sem.at[3 + s]))

        @pl.when((j > 0) & (i == 0))
        def _():
            each(j - 1, lambda copy: copy.wait())

        for r in cuts(BM, RS):
            a = a1[r, :]
            for c in cuts(BN, CS):
                g, u = dot(a, wg[:, c]), dot(a, wu[:, c])
                back = lax.dot_general(dy[r, :], wd[c, :], NT, preferred_element_type=f32).astype(bf16).astype(f32)
                hid[r, c], dgu_o[0, r, c], dgu_o[1, r, c] = gated(g, u, back)
        for k in range(2):
            total[k] = added(i == 0, total[k], lax.dot_general(a1[...], dgu_o[k], TN, preferred_element_type=f32))
        down[...] = added(i == 0, down[...], lax.dot_general(hid[...], dy[...], TN, preferred_element_type=f32))

        def last():
            @pl.when(i == steps - 1)
            def _():
                for x in range(2):
                    leaving[:, x] = total[:, mine(x, 1 - core), :].astype(bf16)
                down_leaving[...] = down[...].astype(bf16)
                each(j, lambda copy: copy.start())

            @pl.when((j == tiles - 1) & (i == steps - 1))
            def _():
                each(j, lambda copy: copy.wait())

        return last

    into = pl.BlockSpec((None, D, BN), lambda j, i, p: (1, 0, at(j)))
    plain = pl.BlockSpec((BM, D), lambda j, i, p: (i, 0))
    return call(
        body,
        place,
        after,
        [
            (a1, plain),
            (dy, plain),
            (w_gate, into),
            (w_up, into),
            (w_down, pl.BlockSpec((None, BN, D), lambda j, i, p: (1, at(j), 0))),
        ],
        [
            (shaped(2, T, F), pl.BlockSpec((2, BM, BN), lambda j, i, p: (0, i, at(j))), held[0]),
            (shaped(2, 2, QD, tiles * BN, dtype=f32), ANY, None),
            (shaped(2, 2, QD, tiles * BN), ANY, None),
            (shaped(2, rows, D, dtype=f32), ANY, held[1]),
            (shaped(2, rows, D), ANY, held[2]),
        ],
        (tiles, steps),
        [
            pltpu.VMEM((2, D, BN), f32),
            pltpu.VMEM((2, 2, QD, BN), bf16),
            pltpu.VMEM((BM, BN), bf16),
            pltpu.VMEM((BN, D), f32),
            pltpu.VMEM((BN, D), bf16),
            pltpu.SemaphoreType.DMA((5,)),
        ],
    )


def send_into_job(keep, came):
    def job(place, keep, came, out):
        out[...] = (keep[...] + came[...].astype(f32)).astype(bf16)

    columns = keep.shape[-1]
    half = pl.BlockSpec((None, None, QD, columns), lambda k, p: (k, 1 - p[0], 0, 0))
    return [(keep, half), (came, half)], [(shaped(2, QD, columns), pl.BlockSpec((None, QD, columns), lambda k, p: (k, 0, 0)), None)], job, ()


def send_down_job(keep, came):
    def job(place, keep, came, out):
        out[...] = (keep[...] + came[...].astype(f32)).astype(bf16)

    rows = keep.shape[1]
    theirs = pl.BlockSpec((None, rows // 2, D), lambda k, p: (1, k, 0))
    return [(keep, theirs), (came, theirs)], [(shaped(rows, D), pl.BlockSpec((rows // 2, D), lambda k, p: (k, 0)), None)], job, ()


def back1(place, after, tile, dgu, dy, h, w_gate, w_up):
    WN = 2 * BN

    def body(place, dgu, wg, wu, h, dy, o, acc):
        j = pl.program_id(0)
        for r in cuts(BM, RS):
            for which, w in enumerate((wg, wu)):
                new = lax.dot_general(dgu[which, r, :], w[...], NT, preferred_element_type=f32)
                acc[which, r, :] = added(j == 0, acc[which, r, :], new)

        def last():
            @pl.when(j == F // WN - 1)
            def _():
                def rows_of(r, _):
                    r = pl.ds(pl.multiple_of(r * 256, 256), 256)
                    da = (acc[0, r, :].astype(bf16) + acc[1, r, :].astype(bf16)).astype(f32)
                    wide = h[r, :].astype(f32)
                    scale = lax.rsqrt(jnp.mean(wide * wide, -1, keepdims=True) + 1e-6)
                    along = jnp.mean(da * wide, -1, keepdims=True)
                    dwide = (da * scale - wide * (along * scale * scale * scale)).astype(bf16)
                    o[r, :] = dy[r, :] + dwide
                    return 0

                lax.fori_loop(0, BM // 256, rows_of, 0)

        return last

    into = pl.BlockSpec((None, D, WN), lambda j, p: (1, 0, j))
    plain = pl.BlockSpec((BM, D), lambda j, p: (tile, 0))
    return call(
        body,
        place,
        after,
        [(dgu, pl.BlockSpec((2, BM, WN), lambda j, p: (0, tile, j))), (w_gate, into), (w_up, into), (h, plain), (dy, plain)],
        [(shaped(BM, D), pl.BlockSpec((BM, D), lambda j, p: (0, 0)), None)],
        (F // WN,),
        [pltpu.VMEM((2, BM, D), f32)],
    )


def back0(place, after, span, dhs, gate, up, aT, w_down, jobs=()):
    first, _, tiles = span
    steps = TT // BM

    def body(place, *refs):
        refs, (g_r, u_r, aT, wd, into_own, into_out, dgu, total, dh, sem) = refs[:steps], refs[steps:]
        j, i = pl.program_id(0), pl.program_id(1)

        def copy(k):
            return pltpu.make_async_copy(refs[k], dh.at[k], sem.at[k])

        @pl.when((j == 0) & (i == 0))
        def _():
            for k in range(steps):
                copy(k).start()

        for k in range(steps):
            pl.when((j == 0) & (i == k))(lambda k=k: copy(k).wait())

        for r in cuts(BM, RS):
            for c in cuts(BN, CS):
                back = lax.dot_general(dh[i, r, :], wd[c, :], NT, preferred_element_type=f32).astype(bf16).astype(f32)
                _, dgu[0, r, c], dgu[1, r, c] = gated(g_r[r, c], u_r[r, c], back)
        for k in range(2):
            total[k] = added(i == 0, total[k], dot(aT[...], dgu[k]))

        def last():
            @pl.when(i == steps - 1)
            def _():
                into_own[...] = total[:, pl.ds(pl.multiple_of(place[1] * QD, QD), QD), :]
                into_out[...] = total[:, pl.ds(pl.multiple_of((1 - place[1]) * QD, QD), QD), :].astype(bf16)

        return last

    wide = pl.BlockSpec((BM, BN), lambda j, i, p: (i, first + j))
    block = pl.BlockSpec((2, QD, BN), lambda j, i, p: (0, 0, j))
    return call(
        body,
        place,
        after,
        [(one, ANY) for one in dhs]
        + [
            (gate, wide),
            (up, wide),
            (aT, pl.BlockSpec((2 * QD, BM), lambda j, i, p: (p[0], i))),
            (w_down, pl.BlockSpec((None, BN, D), lambda j, i, p: (0, first + j, 0))),
        ],
        [(shaped(2, QD, tiles * BN, dtype=f32), block, None), (shaped(2, QD, tiles * BN), block, None)],
        (tiles, steps),
        [
            pltpu.VMEM((2, BM, BN), bf16),
            pltpu.VMEM((2, 2 * QD, BN), f32),
            pltpu.VMEM((steps, BM, D), bf16),
            pltpu.SemaphoreType.DMA((steps,)),
        ],
        jobs,
    )


def grad_down(place, after, hidden, dhs):
    rows = 384
    n = QF // rows

    def tile(i, place):
        return jnp.where(i < n, place[1] * n + i, (1 - place[1]) * n + i - n)

    def body(place, hidden, *refs):
        dhs, (own, out) = refs[:-2], refs[-2:]
        i = pl.program_id(0)
        total = None
        for k, dh in enumerate(dhs):
            term = lax.dot_general(hidden[k * BM : (k + 1) * BM, :], dh[...], TN, preferred_element_type=f32)
            total = term if total is None else total + term

        @pl.when(i < n)
        def _():
            own[...] = total

        @pl.when(i >= n)
        def _():
            out[...] = total.astype(bf16)

    once = pl.Buffered(1)
    return call(
        body,
        place,
        after,
        [(hidden, pl.BlockSpec((TT, rows), lambda i, p: (0, tile(i, p))))]
        + [(one, pl.BlockSpec((BM, D), lambda i, p: (0, 0), pipeline_mode=once)) for one in dhs],
        [
            (shaped(QF, D, dtype=f32), pl.BlockSpec((rows, D), lambda i, p: (jnp.minimum(i, n - 1), 0)), None),
            (shaped(QF, D), pl.BlockSpec((rows, D), lambda i, p: (jnp.maximum(i - n, 0), 0)), None),
        ],
        (2 * n,),
    )


def adamw(g, w, m, v):
    g = g.astype(bf16).astype(f32)
    m = 0.9 * m + 0.1 * g
    v = 0.95 * v + 0.05 * g * g
    return (w - 0.02 * (m * lax.rsqrt(v + 1e-8) + 0.1 * w)).astype(bf16), m, v


def nothing(place):
    pass


def down_job(layer, chunks, own, came, far, w, m, v, held):
    on0, on1, n = chunks

    def job(place, *refs):
        terms, (w, m, v, new_o, m_o, v_o) = refs[:-6], refs[-6:]
        g = sum(term[...].astype(f32) for term in terms)
        new_o[...], m_o[...], v_o[...] = adamw(g, w[...].astype(f32), m[...], v[...])

    def at(s, p):
        return s + jnp.where(p[1] == 0, on0, on1)

    block = pl.BlockSpec((NQ, D), lambda s, p: (s, 0))
    ours = pl.BlockSpec((None, NQ, D), lambda s, p: (0, s, 0)) if far else block
    kept = pl.BlockSpec((None, NQ, D), lambda s, p: (layer, at(s, p), 0))
    whole = pl.BlockSpec((None, NQ, D), lambda s, p: (layer, (2 * p[0] + p[1]) * 3 + at(s, p), 0))
    ins = [(own, ours), (came, ours)] + [(one, block) for one in far] + [(w, whole), (m, kept), (v, kept)]
    outs = [(shaped(n * NQ, D), block, None)]
    outs += [(shaped(2, QF, D, dtype=f32), kept, one) for one in held]
    return ins, outs, job, ()


def into_job(layer, span, parts, ws, ms, vs, held):
    first, stride, tiles = span
    columns = 384
    per = BN // columns
    terms = len(parts)

    def at(s):
        return (first + stride * (s // per)) * per + s % per

    def job(place, *refs):
        parts, refs = refs[:terms], refs[terms:]
        ws, ms, vs = refs[:2], refs[2:4], refs[4:6]
        new, m_o, v_o = refs[6], refs[7:9], refs[9:11]
        for k in range(2):
            g = sum(part[k].astype(f32) for part in parts)
            new[k], m_o[k][...], v_o[k][...] = adamw(g, ws[k][...].astype(f32), ms[k][...], vs[k][...])

    block = pl.BlockSpec((2, QD, columns), lambda s, p: (0, 0, s))
    of_both = pl.BlockSpec((2, None, QD, columns), lambda s, p: (0, p[0], 0, s))
    whole = pl.BlockSpec((None, QD, columns), lambda s, p: (layer, 2 * p[0] + p[1], at(s)))
    kept = pl.BlockSpec((None, QD, columns), lambda s, p: (layer, 0, at(s)))
    ins = [(part, of_both if part.ndim == 4 else block) for part in parts]
    ins += [(w, whole) for w in ws] + [(m, kept) for m in ms] + [(v, kept) for v in vs]
    outs = [(shaped(2, QD, tiles * BN), block, None)] + [(shaped(2, QD, F, dtype=f32), kept, one) for one in held]
    return ins, outs, job, ()


def alone(place, after, grid, jobs):
    return call(nothing, place, after, [], [], grid, jobs=jobs)


def down_pieces(layer, chunks, blocks):
    on0, on1, n = chunks
    rows = n * NQ // 2
    for r, block in enumerate(blocks):
        for h in range(2):

            def there(place, r=r, h=h):
                d = jnp.bitwise_xor(2 * place[0] + place[1], r)
                at = d * QF + jnp.where(lax.rem(d, 2) == 0, on0, on1) * NQ + h * rows
                return layer, pl.ds(pl.multiple_of(at, 192), rows), slice(None)

            yield block, (slice(h * rows, (h + 1) * rows), slice(None)), "down", there


def into_pieces(layer, span, blocks):
    first, stride, tiles = span
    if stride == 1:
        places = [(0, first, tiles)]
    else:
        places = [(j, first + stride * j, 1) for j in range(tiles)]
    for r, block in enumerate(blocks):
        for k, name in enumerate(("gate", "up")):
            for here, to, n in places:

                def there(place, r=r, to=to, n=n):
                    d = jnp.bitwise_xor(2 * place[0] + place[1], r)
                    return layer, pl.ds(pl.multiple_of(d * QD, QD), QD), slice(to * BN, (to + n) * BN)

                yield block, (k, slice(None), slice(here * BN, (here + n) * BN)), name, there


def copy_job(grid, q, pieces, held):
    pieces = list(pieces)
    sources, names = [], []
    for block, _, name, _ in pieces:
        if not any(block is one for one in sources):
            sources.append(block)
        if name not in names:
            names.append(name)
    block, part, _, _ = pieces[0]
    shape = jax.eval_shape(lambda b: b[part], block).shape
    groups = [pieces[at : at + q] for at in range(0, len(pieces), q)]
    steps = grid[0] * (grid[1] if len(grid) > 1 else 1)
    assert steps >= len(groups) + 2

    def body(place, *refs):
        outs, (buffer, reads, writes) = dict(zip(names, refs[len(sources) : -3], strict=True)), refs[-3:]
        step = pl.program_id(0) if len(grid) == 1 else pl.program_id(0) * grid[1] + pl.program_id(1)

        def copies(g):
            for n, (block, part, name, there) in enumerate(groups[g]):
                source = refs[next(k for k, one in enumerate(sources) if one is block)]
                slot = (g % 2) * q + n
                yield (
                    functools.partial(pltpu.make_async_copy, source.at[part], buffer.at[slot], reads.at[slot]),
                    functools.partial(pltpu.make_async_copy, buffer.at[slot], outs[name].at[there(place)], writes.at[slot]),
                )

        for s in range(len(groups) + 2):

            @pl.when(step == s)
            def _(s=s):
                if s >= 2:
                    for _, write in copies(s - 2):
                        write().wait()
                if s < len(groups):
                    for read, _ in copies(s):
                        read().start()
                if 1 <= s <= len(groups):
                    for read, write in copies(s - 1):
                        read().wait()
                        write().start()

    body.copies = True
    whole = {"gate": shaped(2, D, F), "up": shaped(2, D, F), "down": shaped(2, F, D)}
    outs = [(whole[name], ANY, held[name]) for name in names]
    scratch = (pltpu.VMEM((2 * q,) + shape, bf16), pltpu.SemaphoreType.DMA((2 * q,)), pltpu.SemaphoreType.DMA((2 * q,)))
    return [(one, ANY) for one in sources], outs, body, scratch


def spread(new):
    far = over(new, OVER_X)
    near = over(new, OVER_CORE)
    return [new, near, far, over(far, OVER_CORE)]


def whole_step(x, dy, w_gate, w_up, w_down, m_gate, m_up, m_down, v_gate, v_up, v_down):
    d = lax.axis_index("dp")
    place = jnp.stack([d // 2, d % 2]).astype(jnp.int32)
    x, dy = x[0], dy[0]
    x_far = over(x, OVER_X)

    weights = (w_gate, w_up, w_down)
    (gate, up, hid0, aT0, h, a1), t = forward0(place, None, 0, x, *weights, [None] * 4, True)

    mv = {"into": (None,) * 4, "down": (None,) * 2}
    ALL, ONE, TWO = (0, 0, 3), (2, 0, 1), (0, 1, 2)

    def into(layer, span, *parts):
        return into_job(layer, span, parts, (w_gate, w_up), (m_gate, m_up), (v_gate, v_up), mv["into"])

    def down(layer, chunks, own, came, *far):
        return down_job(layer, chunks, own, came, far, w_down, m_down, v_down, mv["down"])

    def took(results, kind):
        new, *mv[kind] = results
        return spread(new)

    dgu = None
    terms, new1 = {}, {}

    SPANS = {"p": (1, 1, 1), "q": (4, 1, 1), "r": (0, 3, 1), "s": (3, 3, 1), "u": (2, 3, 1), "v": (5, 3, 1)}

    def gradients(t, name, held_down):
        nonlocal dgu
        (dgu, keep, out, *downs), t = layer1(place, t, SPANS[name], a1, dy, *weights, [dgu, *held_down])
        terms[name] = [keep, over(out, OVER_CORE)]
        return t, downs

    def send(t, name, downs=None):
        jobs = [send_into_job(*terms[name])]
        if downs is not None:
            downs[1] = over(downs[1], OVER_CORE)
            jobs.append(send_down_job(*downs))
        results, t = call(nothing, place, t, [], [], (2,), jobs=jobs)
        terms[name].append(over(results[0], OVER_X))
        if downs is not None:
            downs.append(over(results[1], OVER_X))
        return t

    def adam(t, name):
        span = SPANS[name]
        results, t = alone(place, t, (2 * span[2],), [into(1, span, *terms[name])])
        new1[name] = took(results, "into")
        return t

    def adam_down(t, chunks, downs):
        results, t = alone(place, t, (chunks[2],), [down(1, chunks, *downs)])
        return took(results, "down"), t

    t, downs1 = gradients(t, "p", (None, None))
    t = send(t, "p")
    t, downs1 = gradients(t, "q", downs1)
    t = adam(t, "p")
    t = send(t, "q", downs1)
    t, downs2 = gradients(t, "r", (None, None))
    t = adam(t, "q")
    t = send(t, "r")
    t, downs2 = gradients(t, "s", downs2)
    down1, t = adam_down(t, ONE, downs1)
    t = send(t, "s")
    t = adam(t, "r")
    t, downs2 = gradients(t, "u", downs2)
    t = adam(t, "s")
    t = send(t, "u")
    t, downs2 = gradients(t, "v", downs2)
    t = adam(t, "u")
    t = send(t, "v", downs2)
    dhs, dhs_far = [], []
    for tile in range(T // BM):
        (dh,), t = back1(place, t, tile, dgu, dy, h, w_gate, w_up)
        dhs.append(dh)
        dhs_far.append(over(dh, OVER_X))
    dhs += dhs_far
    t = adam(t, "v")
    (gate, up, hid0, aT0), t = forward0(place, t, T // BM, x_far, *weights, [gate, up, hid0, aT0], False)

    weights_out = {"gate": None, "up": None, "down": None}

    def copying(grid, q, pieces):
        return copy_job(grid, q, pieces, weights_out)

    def copied(results, names):
        weights_out.update(zip(names, results, strict=True))

    (own_d, out_d), t = grad_down(place, t, hid0, dhs)
    came_d = over(out_d, OVER_CORE)
    down2, t = adam_down(t, TWO, downs2)
    results, t = alone(place, t, (3,), [down(0, ALL, own_d, came_d)])
    down0 = took(results, "down")

    def first_pieces(*names):
        return [piece for name in names for piece in into_pieces(1, SPANS[name], new1[name])]

    new0 = {}
    spans = {"a": (0, 1, 3), "c": (3, 1, 2), "e": (5, 1, 1)}
    beside = {
        "a": lambda: [copying((3, 4), 3, first_pieces("p", "q", "r")), copying((3, 4), 1, down_pieces(1, ONE, down1))],
        "c": lambda: [copying((2, 4), 4, first_pieces("s", "u", "v")), copying((2, 4), 2, down_pieces(1, TWO, down2))],
        "e": lambda: [copying((1, 4), 4, down_pieces(0, ALL, down0))],
    }
    for name, span in spans.items():
        (own, out, *results), t = back0(place, t, span, dhs, gate, up, aT0, w_down, beside[name]())
        copied(results, ("gate", "up", "down")[: len(results)] if name != "e" else ("down",))
        came = over(out, OVER_CORE)
        results, t = alone(place, t, (2 * span[2],), [into(0, span, own, came)])
        new0[name] = took(results, "into")

    for name, q in (("a", 4), ("c", 8), ("e", 8)):
        grid = (8 // q + 2,)
        jobs = [copying(grid, q, into_pieces(0, spans[name], new0[name]))]
        results, t = call(nothing, place, t, [], [], grid, jobs=jobs)
        copied(results, ("gate", "up", "down")[: len(results)])
    held, o_down = (weights_out["gate"], weights_out["up"]), weights_out["down"]
    (m_gate, m_up, v_gate, v_up), (m_down, v_down) = mv["into"], mv["down"]
    return *held, o_down, m_gate, m_up, m_down, v_gate, v_up, v_down


def solution(mesh):
    sequences, whole = P(("rep", "dp"), None, None), P(None, None, None)
    block, group, own = P(None, "dp", None), P("rep", None, None), P("rep", "dp", None)
    return jax.shard_map(
        whole_step,
        mesh=mesh,
        in_specs=(sequences,) * 2 + (whole,) * 3 + (block,) * 6,
        out_specs=(group,) * 3 + (own,) * 6,
        check_vma=False,
    )
```

```python
import functools

import jax
import jax.numpy as jnp
from jax import lax
from jax.experimental import pallas as pl
from jax.experimental.pallas import tpu as pltpu
from jax.sharding import PartitionSpec as P


f32, bf16 = jnp.float32, jnp.bfloat16
T, D, F = 2048, 1152, 4608
TT = 2 * T
HALF = F // 2
BM, BN = 1024, 768
NF, NH = F // BN, HALF // BN
RS, CS = 512, 256
NQ = 384
VMEM = 67043328
QD, QF = D // 4, F // 4
ANY = pl.BlockSpec(memory_space=pl.ANY)
TOKEN = jax.ShapeDtypeStruct((8, 128), jnp.int32)
NT = (((1,), (1,)), ((), ()))
TN = (((0,), (0,)), ((), ()))

OVER_X = [(d, d ^ 2) for d in range(4)]
OVER_CORE = [(d, d ^ 1) for d in range(4)]


def over(array, pairs):
    return lax.ppermute(array, "dp", pairs)


def sigmoid(g):
    return 0.5 * jnp.tanh(0.5 * g) + 0.5


def cuts(n, size):
    return [slice(at, at + size) for at in range(0, n, size)]


def added(first, total, new):
    return jnp.where(first, 0.0, total) + new


def gated(g, u, back):
    s = sigmoid(g)
    silu = g * s
    return (silu * u).astype(bf16), (back * u * (s + silu * (1 - s))).astype(bf16), (back * silu).astype(bf16)


def dot(a, b):
    return jnp.dot(a, b, preferred_element_type=f32)


def call(body, place, after, ins, outs, grid, scratch=(), jobs=()):
    bodies = [(body, len(ins), len(outs), len(scratch))] + [(job, len(i), len(o), len(s)) for i, o, job, s in jobs]
    ins = list(ins) + [one for i, _, _, _ in jobs for one in i]
    outs = list(outs) + [one for _, o, _, _ in jobs for one in o]
    scratch = list(scratch) + [one for _, _, _, s in jobs for one in s]
    arrays = [a for a, _ in ins]
    specs = [s for _, s in ins]
    aliases = {}
    held = [(k, buffer) for k, (_, _, buffer) in enumerate(outs) if buffer is not None]
    for n, (k, buffer) in enumerate(held):
        aliases[1 + len(arrays) + n] = k
    arrays += [buffer for _, buffer in held]
    specs += [ANY] * len(held)
    if after is not None:
        arrays.append(after)
        specs.append(ANY)
    skip = len(arrays) - len(ins)

    def kernel(place_ref, *refs):
        refs, rest = refs[: len(ins)], refs[len(ins) + skip :]
        results, token, own = rest[: len(outs)], rest[len(outs)], rest[len(outs) + 1 :]
        token[...] = jnp.zeros_like(token)
        parts = []
        at_in = at_out = at = 0
        for one, n_in, n_out, n in bodies:
            mine = (*refs[at_in : at_in + n_in], *results[at_out : at_out + n_out], *own[at : at + n])
            parts.append(functools.partial(one, place_ref, *mine))
            at_in, at_out, at = at_in + n_in, at_out + n_out, at + n
        for part, (one, *_) in zip(parts, bodies, strict=True):
            if getattr(one, "copies", False):
                part()
        last = [part() for part, (one, *_) in zip(parts, bodies, strict=True) if not getattr(one, "copies", False)]
        if last[0] is not None:
            last[0]()

    result = pl.pallas_call(
        kernel,
        grid_spec=pltpu.PrefetchScalarGridSpec(
            num_scalar_prefetch=1,
            grid=grid,
            in_specs=specs,
            out_specs=[s for _, s, _ in outs] + [pl.BlockSpec((8, 128), lambda *_: (0, 0))],
            scratch_shapes=scratch,
        ),
        out_shape=[o for o, _, _ in outs] + [TOKEN],
        input_output_aliases=aliases,
        cost_estimate=pl.CostEstimate(flops=T * D * F, bytes_accessed=T * D * F, transcendentals=0),
        compiler_params=pltpu.CompilerParams(vmem_limit_bytes=VMEM),
    )(place, *arrays)
    return result[:-1], result[-1]


def shaped(*shape, dtype=bf16):
    return jax.ShapeDtypeStruct(shape, dtype)


def normalise(h, a):
    def rows_of(i, _):
        rows = pl.ds(pl.multiple_of(i * 256, 256), 256)
        wide = h[rows, :].astype(f32)
        scale = lax.rsqrt(jnp.mean(wide * wide, -1, keepdims=True) + 1e-6)
        a[rows, :] = (wide * scale).astype(bf16)
        return 0

    lax.fori_loop(0, h.shape[0] // 256, rows_of, 0)


def forward0(place, after, first, x, w_gate, w_up, w_down, held, whole):
    rows = x.shape[0]

    def tile(j, place):
        return jnp.where(j < NH, place[0] * NH + j, (1 - place[0]) * NH + j - NH)

    def body(place, x, wg, wu, *refs):
        if whole:
            wd, g_o, u_o, hid_o, aT_o, h_o, a1_o, a_s, hs, acc = refs
        else:
            g_o, u_o, hid_o, aT_o, a_s, hs = refs
        j = pl.program_id(1)

        @pl.when(j == 0)
        def _():
            normalise(x, a_s)

        part = pl.ds(pl.multiple_of(jnp.minimum(j * 256, BM - 256), 256), 256)
        aT_o[:, part] = a_s[part, :].T
        for r in cuts(BM, RS):
            a = a_s[r, :]
            for c in cuts(BN, CS):
                g, u = dot(a, wg[:, c]), dot(a, wu[:, c])
                g_o[r, c] = g
                u_o[r, c] = u
                hs[r, c] = (g * sigmoid(g) * u).astype(bf16)
            if whole:
                acc[r, :] = added(j == 0, acc[r, :], dot(hs[r, :], wd[...]))

        @pl.when(j < NH)
        def _():
            hid_o[...] = hs[...]

        if whole:

            @pl.when(j == NF - 1)
            def _():
                def rows_of(i, _):
                    rows = pl.ds(pl.multiple_of(i * 256, 256), 256)
                    h_o[rows, :] = x[rows, :] + acc[rows, :].astype(bf16)
                    return 0

                lax.fori_loop(0, BM // 256, rows_of, 0)
                normalise(h_o, a1_o)

    wide = pl.BlockSpec((BM, BN), lambda i, j, p: (first + i, tile(j, p)))
    into = pl.BlockSpec((None, D, BN), lambda i, j, p: (0, 0, tile(j, p)))
    plain = pl.BlockSpec((BM, D), lambda i, j, p: (i, 0))
    ins = [(x, plain), (w_gate, into), (w_up, into)]
    outs = [
        (shaped(TT, F, dtype=f32), wide, held[0]),
        (shaped(TT, F, dtype=f32), wide, held[1]),
        (shaped(TT, HALF), pl.BlockSpec((BM, BN), lambda i, j, p: (first + i, jnp.minimum(j, NH - 1))), held[2]),
        (shaped(D, TT), pl.BlockSpec((D, BM), lambda i, j, p: (0, first + i)), held[3]),
    ]
    scratch = [pltpu.VMEM((BM, D), bf16), pltpu.VMEM((BM, BN), bf16)]
    if whole:
        ins += [(w_down, pl.BlockSpec((None, BN, D), lambda i, j, p: (0, tile(j, p), 0)))]
        outs += [(shaped(T, D), plain, None), (shaped(T, D), plain, None)]
        scratch += [pltpu.VMEM((BM, D), f32)]
    return call(body, place, after, ins, outs, (rows // BM, NF), scratch)


def layer1(place, after, span, a1, dy, w_gate, w_up, w_down, held):
    steps = T // BM
    first, stride, tiles = span
    t = first % NH
    rows = NQ if t == 1 else 2 * NQ

    def at(j):
        return first + stride * j

    def body(place, a1, dy, wg, wu, wd, dgu_o, keep, out, down_keep, down_out, total, leaving, hid, down, down_leaving, sem):
        j, i = pl.program_id(0), pl.program_id(1)
        core = place[1]

        def mine(x, core):
            return pl.ds(pl.multiple_of((2 * x + core) * QD, QD), QD)

        def each(j, act):
            side = jnp.where(place[0] == at(j) // NH, 0, 1)
            columns = pl.ds(pl.multiple_of(j * BN, BN), BN)
            for x in range(2):
                act(pltpu.make_async_copy(total.at[:, mine(x, core), :], keep.at[:, x, :, columns], sem.at[x]))
            act(pltpu.make_async_copy(leaving, out.at[:, :, :, columns], sem.at[2]))
            for s in range(2):
                owner = (2 * t + s) // 3
                here, to = pl.ds(s * NQ, NQ), pl.ds(0 if t == 1 else s * NQ, NQ)

                @pl.when(core == owner)
                def _():
                    act(pltpu.make_async_copy(down.at[here, :], down_keep.at[side, to, :], sem.at[3 + s]))

                @pl.when(core != owner)
                def _():
                    act(pltpu.make_async_copy(down_leaving.at[here, :], down_out.at[side, to, :], sem.at[3 + s]))

        @pl.when((j > 0) & (i == 0))
        def _():
            each(j - 1, lambda copy: copy.wait())

        for r in cuts(BM, RS):
            a = a1[r, :]
            for c in cuts(BN, CS):
                g, u = dot(a, wg[:, c]), dot(a, wu[:, c])
                back = lax.dot_general(dy[r, :], wd[c, :], NT, preferred_element_type=f32).astype(bf16).astype(f32)
                hid[r, c], dgu_o[0, r, c], dgu_o[1, r, c] = gated(g, u, back)
        for k in range(2):
            total[k] = added(i == 0, total[k], lax.dot_general(a1[...], dgu_o[k], TN, preferred_element_type=f32))
        down[...] = added(i == 0, down[...], lax.dot_general(hid[...], dy[...], TN, preferred_element_type=f32))

        def last():
            @pl.when(i == steps - 1)
            def _():
                for x in range(2):
                    leaving[:, x] = total[:, mine(x, 1 - core), :].astype(bf16)
                down_leaving[...] = down[...].astype(bf16)
                each(j, lambda copy: copy.start())

            @pl.when((j == tiles - 1) & (i == steps - 1))
            def _():
                each(j, lambda copy: copy.wait())

        return last

    into = pl.BlockSpec((None, D, BN), lambda j, i, p: (1, 0, at(j)))
    plain = pl.BlockSpec((BM, D), lambda j, i, p: (i, 0))
    return call(
        body,
        place,
        after,
        [
            (a1, plain),
            (dy, plain),
            (w_gate, into),
            (w_up, into),
            (w_down, pl.BlockSpec((None, BN, D), lambda j, i, p: (1, at(j), 0))),
        ],
        [
            (shaped(2, T, F), pl.BlockSpec((2, BM, BN), lambda j, i, p: (0, i, at(j))), held[0]),
            (shaped(2, 2, QD, tiles * BN, dtype=f32), ANY, None),
            (shaped(2, 2, QD, tiles * BN), ANY, None),
            (shaped(2, rows, D, dtype=f32), ANY, held[1]),
            (shaped(2, rows, D), ANY, held[2]),
        ],
        (tiles, steps),
        [
            pltpu.VMEM((2, D, BN), f32),
            pltpu.VMEM((2, 2, QD, BN), bf16),
            pltpu.VMEM((BM, BN), bf16),
            pltpu.VMEM((BN, D), f32),
            pltpu.VMEM((BN, D), bf16),
            pltpu.SemaphoreType.DMA((5,)),
        ],
    )


def send_into_job(keep, came):
    def job(place, keep, came, out):
        out[...] = (keep[...] + came[...].astype(f32)).astype(bf16)

    columns = keep.shape[-1]
    half = pl.BlockSpec((None, None, QD, columns), lambda k, p: (k, 1 - p[0], 0, 0))
    return [(keep, half), (came, half)], [(shaped(2, QD, columns), pl.BlockSpec((None, QD, columns), lambda k, p: (k, 0, 0)), None)], job, ()


def send_down_job(keep, came):
    def job(place, keep, came, out):
        out[...] = (keep[...] + came[...].astype(f32)).astype(bf16)

    rows = keep.shape[1]
    theirs = pl.BlockSpec((None, rows // 2, D), lambda k, p: (1, k, 0))
    return [(keep, theirs), (came, theirs)], [(shaped(rows, D), pl.BlockSpec((rows // 2, D), lambda k, p: (k, 0)), None)], job, ()


def back1(place, after, tile, dgu, dy, h, w_gate, w_up):
    WN = 2 * BN

    def body(place, dgu, wg, wu, h, dy, o, acc):
        j = pl.program_id(0)
        for r in cuts(BM, RS):
            for which, w in enumerate((wg, wu)):
                new = lax.dot_general(dgu[which, r, :], w[...], NT, preferred_element_type=f32)
                acc[which, r, :] = added(j == 0, acc[which, r, :], new)

        def last():
            @pl.when(j == F // WN - 1)
            def _():
                def rows_of(r, _):
                    r = pl.ds(pl.multiple_of(r * 256, 256), 256)
                    da = (acc[0, r, :].astype(bf16) + acc[1, r, :].astype(bf16)).astype(f32)
                    wide = h[r, :].astype(f32)
                    scale = lax.rsqrt(jnp.mean(wide * wide, -1, keepdims=True) + 1e-6)
                    along = jnp.mean(da * wide, -1, keepdims=True)
                    dwide = (da * scale - wide * (along * scale * scale * scale)).astype(bf16)
                    o[r, :] = dy[r, :] + dwide
                    return 0

                lax.fori_loop(0, BM // 256, rows_of, 0)

        return last

    into = pl.BlockSpec((None, D, WN), lambda j, p: (1, 0, j))
    plain = pl.BlockSpec((BM, D), lambda j, p: (tile, 0))
    return call(
        body,
        place,
        after,
        [(dgu, pl.BlockSpec((2, BM, WN), lambda j, p: (0, tile, j))), (w_gate, into), (w_up, into), (h, plain), (dy, plain)],
        [(shaped(BM, D), pl.BlockSpec((BM, D), lambda j, p: (0, 0)), None)],
        (F // WN,),
        [pltpu.VMEM((2, BM, D), f32)],
    )


def back0(place, after, span, dhs, gate, up, aT, w_down, jobs=()):
    first, _, tiles = span
    steps = TT // BM

    def body(place, *refs):
        refs, (g_r, u_r, aT, wd, into_own, into_out, dgu, total, dh, sem) = refs[:steps], refs[steps:]
        j, i = pl.program_id(0), pl.program_id(1)

        def copy(k):
            return pltpu.make_async_copy(refs[k], dh.at[k], sem.at[k])

        @pl.when((j == 0) & (i == 0))
        def _():
            for k in range(steps):
                copy(k).start()

        for k in range(steps):
            pl.when((j == 0) & (i == k))(lambda k=k: copy(k).wait())

        for r in cuts(BM, RS):
            for c in cuts(BN, CS):
                back = lax.dot_general(dh[i, r, :], wd[c, :], NT, preferred_element_type=f32).astype(bf16).astype(f32)
                _, dgu[0, r, c], dgu[1, r, c] = gated(g_r[r, c], u_r[r, c], back)
        for k in range(2):
            total[k] = added(i == 0, total[k], dot(aT[...], dgu[k]))

        def last():
            @pl.when(i == steps - 1)
            def _():
                into_own[...] = total[:, pl.ds(pl.multiple_of(place[1] * QD, QD), QD), :]
                into_out[...] = total[:, pl.ds(pl.multiple_of((1 - place[1]) * QD, QD), QD), :].astype(bf16)

        return last

    wide = pl.BlockSpec((BM, BN), lambda j, i, p: (i, first + j))
    block = pl.BlockSpec((2, QD, BN), lambda j, i, p: (0, 0, j))
    return call(
        body,
        place,
        after,
        [(one, ANY) for one in dhs]
        + [
            (gate, wide),
            (up, wide),
            (aT, pl.BlockSpec((2 * QD, BM), lambda j, i, p: (p[0], i))),
            (w_down, pl.BlockSpec((None, BN, D), lambda j, i, p: (0, first + j, 0))),
        ],
        [(shaped(2, QD, tiles * BN, dtype=f32), block, None), (shaped(2, QD, tiles * BN), block, None)],
        (tiles, steps),
        [
            pltpu.VMEM((2, BM, BN), bf16),
            pltpu.VMEM((2, 2 * QD, BN), f32),
            pltpu.VMEM((steps, BM, D), bf16),
            pltpu.SemaphoreType.DMA((steps,)),
        ],
        jobs,
    )


def grad_down(place, after, hidden, dhs):
    rows = 384
    n = QF // rows

    def tile(i, place):
        return jnp.where(i < n, place[1] * n + i, (1 - place[1]) * n + i - n)

    def body(place, hidden, *refs):
        dhs, (own, out) = refs[:-2], refs[-2:]
        i = pl.program_id(0)
        total = None
        for k, dh in enumerate(dhs):
            term = lax.dot_general(hidden[k * BM : (k + 1) * BM, :], dh[...], TN, preferred_element_type=f32)
            total = term if total is None else total + term

        @pl.when(i < n)
        def _():
            own[...] = total

        @pl.when(i >= n)
        def _():
            out[...] = total.astype(bf16)

    once = pl.Buffered(1)
    return call(
        body,
        place,
        after,
        [(hidden, pl.BlockSpec((TT, rows), lambda i, p: (0, tile(i, p))))]
        + [(one, pl.BlockSpec((BM, D), lambda i, p: (0, 0), pipeline_mode=once)) for one in dhs],
        [
            (shaped(QF, D, dtype=f32), pl.BlockSpec((rows, D), lambda i, p: (jnp.minimum(i, n - 1), 0)), None),
            (shaped(QF, D), pl.BlockSpec((rows, D), lambda i, p: (jnp.maximum(i - n, 0), 0)), None),
        ],
        (2 * n,),
    )


def adamw(g, w, m, v):
    g = g.astype(bf16).astype(f32)
    m = 0.9 * m + 0.1 * g
    v = 0.95 * v + 0.05 * g * g
    return (w - 0.02 * (m * lax.rsqrt(v + 1e-8) + 0.1 * w)).astype(bf16), m, v


def nothing(place):
    pass


def down_job(layer, chunks, own, came, far, w, m, v, held):
    on0, on1, n = chunks

    def job(place, *refs):
        terms, (w, m, v, new_o, m_o, v_o) = refs[:-6], refs[-6:]
        g = sum(term[...].astype(f32) for term in terms)
        new_o[...], m_o[...], v_o[...] = adamw(g, w[...].astype(f32), m[...], v[...])

    def at(s, p):
        return s + jnp.where(p[1] == 0, on0, on1)

    block = pl.BlockSpec((NQ, D), lambda s, p: (s, 0))
    ours = pl.BlockSpec((None, NQ, D), lambda s, p: (0, s, 0)) if far else block
    kept = pl.BlockSpec((None, NQ, D), lambda s, p: (layer, at(s, p), 0))
    whole = pl.BlockSpec((None, NQ, D), lambda s, p: (layer, (2 * p[0] + p[1]) * 3 + at(s, p), 0))
    ins = [(own, ours), (came, ours)] + [(one, block) for one in far] + [(w, whole), (m, kept), (v, kept)]
    outs = [(shaped(n * NQ, D), block, None)]
    outs += [(shaped(2, QF, D, dtype=f32), kept, one) for one in held]
    return ins, outs, job, ()


def into_job(layer, span, parts, ws, ms, vs, held):
    first, stride, tiles = span
    columns = 384
    per = BN // columns
    terms = len(parts)

    def at(s):
        return (first + stride * (s // per)) * per + s % per

    def job(place, *refs):
        parts, refs = refs[:terms], refs[terms:]
        ws, ms, vs = refs[:2], refs[2:4], refs[4:6]
        new, m_o, v_o = refs[6], refs[7:9], refs[9:11]
        for k in range(2):
            g = sum(part[k].astype(f32) for part in parts)
            new[k], m_o[k][...], v_o[k][...] = adamw(g, ws[k][...].astype(f32), ms[k][...], vs[k][...])

    block = pl.BlockSpec((2, QD, columns), lambda s, p: (0, 0, s))
    of_both = pl.BlockSpec((2, None, QD, columns), lambda s, p: (0, p[0], 0, s))
    whole = pl.BlockSpec((None, QD, columns), lambda s, p: (layer, 2 * p[0] + p[1], at(s)))
    kept = pl.BlockSpec((None, QD, columns), lambda s, p: (layer, 0, at(s)))
    ins = [(part, of_both if part.ndim == 4 else block) for part in parts]
    ins += [(w, whole) for w in ws] + [(m, kept) for m in ms] + [(v, kept) for v in vs]
    outs = [(shaped(2, QD, tiles * BN), block, None)] + [(shaped(2, QD, F, dtype=f32), kept, one) for one in held]
    return ins, outs, job, ()


def alone(place, after, grid, jobs):
    return call(nothing, place, after, [], [], grid, jobs=jobs)


def down_pieces(layer, chunks, blocks):
    on0, on1, n = chunks
    rows = n * NQ // 2
    for r, block in enumerate(blocks):
        for h in range(2):

            def there(place, r=r, h=h):
                d = jnp.bitwise_xor(2 * place[0] + place[1], r)
                at = d * QF + jnp.where(lax.rem(d, 2) == 0, on0, on1) * NQ + h * rows
                return layer, pl.ds(pl.multiple_of(at, 192), rows), slice(None)

            yield block, (slice(h * rows, (h + 1) * rows), slice(None)), "down", there


def into_pieces(layer, span, blocks):
    first, stride, tiles = span
    if stride == 1:
        places = [(0, first, tiles)]
    else:
        places = [(j, first + stride * j, 1) for j in range(tiles)]
    for r, block in enumerate(blocks):
        for k, name in enumerate(("gate", "up")):
            for here, to, n in places:

                def there(place, r=r, to=to, n=n):
                    d = jnp.bitwise_xor(2 * place[0] + place[1], r)
                    return layer, pl.ds(pl.multiple_of(d * QD, QD), QD), slice(to * BN, (to + n) * BN)

                yield block, (k, slice(None), slice(here * BN, (here + n) * BN)), name, there


def copy_job(grid, q, pieces, held):
    pieces = list(pieces)
    sources, names = [], []
    for block, _, name, _ in pieces:
        if not any(block is one for one in sources):
            sources.append(block)
        if name not in names:
            names.append(name)
    block, part, _, _ = pieces[0]
    shape = jax.eval_shape(lambda b: b[part], block).shape
    groups = [pieces[at : at + q] for at in range(0, len(pieces), q)]
    steps = grid[0] * (grid[1] if len(grid) > 1 else 1)
    assert steps >= len(groups) + 2

    def body(place, *refs):
        outs, (buffer, reads, writes) = dict(zip(names, refs[len(sources) : -3], strict=True)), refs[-3:]
        step = pl.program_id(0) if len(grid) == 1 else pl.program_id(0) * grid[1] + pl.program_id(1)

        def copies(g):
            for n, (block, part, name, there) in enumerate(groups[g]):
                source = refs[next(k for k, one in enumerate(sources) if one is block)]
                slot = (g % 2) * q + n
                yield (
                    functools.partial(pltpu.make_async_copy, source.at[part], buffer.at[slot], reads.at[slot]),
                    functools.partial(pltpu.make_async_copy, buffer.at[slot], outs[name].at[there(place)], writes.at[slot]),
                )

        for s in range(len(groups) + 2):

            @pl.when(step == s)
            def _(s=s):
                if s >= 2:
                    for _, write in copies(s - 2):
                        write().wait()
                if s < len(groups):
                    for read, _ in copies(s):
                        read().start()
                if 1 <= s <= len(groups):
                    for read, write in copies(s - 1):
                        read().wait()
                        write().start()

    body.copies = True
    whole = {"gate": shaped(2, D, F), "up": shaped(2, D, F), "down": shaped(2, F, D)}
    outs = [(whole[name], ANY, held[name]) for name in names]
    scratch = (pltpu.VMEM((2 * q,) + shape, bf16), pltpu.SemaphoreType.DMA((2 * q,)), pltpu.SemaphoreType.DMA((2 * q,)))
    return [(one, ANY) for one in sources], outs, body, scratch


def spread(new):
    far = over(new, OVER_X)
    near = over(new, OVER_CORE)
    return [new, near, far, over(far, OVER_CORE)]


def whole_step(x, dy, w_gate, w_up, w_down, m_gate, m_up, m_down, v_gate, v_up, v_down):
    d = lax.axis_index("dp")
    place = jnp.stack([d // 2, d % 2]).astype(jnp.int32)
    x, dy = x[0], dy[0]
    x_far = over(x, OVER_X)

    weights = (w_gate, w_up, w_down)
    (gate, up, hid0, aT0, h, a1), t = forward0(place, None, 0, x, *weights, [None] * 4, True)

    mv = {"into": (None,) * 4, "down": (None,) * 2}
    ALL, ONE, TWO = (0, 0, 3), (2, 0, 1), (0, 1, 2)

    def into(layer, span, *parts):
        return into_job(layer, span, parts, (w_gate, w_up), (m_gate, m_up), (v_gate, v_up), mv["into"])

    def down(layer, chunks, own, came, *far):
        return down_job(layer, chunks, own, came, far, w_down, m_down, v_down, mv["down"])

    def took(results, kind):
        new, *mv[kind] = results
        return spread(new)

    dgu = None
    terms, new1 = {}, {}

    SPANS = {"p": (1, 1, 1), "q": (4, 1, 1), "r": (0, 3, 1), "s": (3, 3, 1), "u": (2, 3, 1), "v": (5, 3, 1)}

    def gradients(t, name, held_down):
        nonlocal dgu
        (dgu, keep, out, *downs), t = layer1(place, t, SPANS[name], a1, dy, *weights, [dgu, *held_down])
        terms[name] = [keep, over(out, OVER_CORE)]
        return t, downs

    def send(t, name, downs=None):
        jobs = [send_into_job(*terms[name])]
        if downs is not None:
            downs[1] = over(downs[1], OVER_CORE)
            jobs.append(send_down_job(*downs))
        results, t = call(nothing, place, t, [], [], (2,), jobs=jobs)
        terms[name].append(over(results[0], OVER_X))
        if downs is not None:
            downs.append(over(results[1], OVER_X))
        return t

    def adam(t, name):
        span = SPANS[name]
        results, t = alone(place, t, (2 * span[2],), [into(1, span, *terms[name])])
        new1[name] = took(results, "into")
        return t

    def adam_down(t, chunks, downs):
        results, t = alone(place, t, (chunks[2],), [down(1, chunks, *downs)])
        return took(results, "down"), t

    t, downs1 = gradients(t, "p", (None, None))
    t = send(t, "p")
    t, downs1 = gradients(t, "q", downs1)
    t = adam(t, "p")
    t = send(t, "q", downs1)
    t, downs2 = gradients(t, "r", (None, None))
    t = adam(t, "q")
    t = send(t, "r")
    t, downs2 = gradients(t, "s", downs2)
    down1, t = adam_down(t, ONE, downs1)
    t = send(t, "s")
    t = adam(t, "r")
    t, downs2 = gradients(t, "u", downs2)
    t = adam(t, "s")
    t = send(t, "u")
    t, downs2 = gradients(t, "v", downs2)
    t = adam(t, "u")
    t = send(t, "v", downs2)
    dhs, dhs_far = [], []
    for tile in range(T // BM):
        (dh,), t = back1(place, t, tile, dgu, dy, h, w_gate, w_up)
        dhs.append(dh)
        dhs_far.append(over(dh, OVER_X))
    dhs += dhs_far
    t = adam(t, "v")
    (gate, up, hid0, aT0), t = forward0(place, t, T // BM, x_far, *weights, [gate, up, hid0, aT0], False)

    weights_out = {"gate": None, "up": None, "down": None}

    def copying(grid, q, pieces):
        return copy_job(grid, q, pieces, weights_out)

    def copied(results, names):
        weights_out.update(zip(names, results, strict=True))

    (own_d, out_d), t = grad_down(place, t, hid0, dhs)
    came_d = over(out_d, OVER_CORE)
    down2, t = adam_down(t, TWO, downs2)
    results, t = alone(place, t, (3,), [down(0, ALL, own_d, came_d)])
    down0 = took(results, "down")

    def first_pieces(*names):
        return [piece for name in names for piece in into_pieces(1, SPANS[name], new1[name])]

    new0 = {}
    spans = {"a": (0, 1, 3), "c": (3, 1, 2), "e": (5, 1, 1)}
    beside = {
        "a": lambda: [copying((3, 4), 3, first_pieces("p", "q", "r")), copying((3, 4), 1, down_pieces(1, ONE, down1))],
        "c": lambda: [copying((2, 4), 4, first_pieces("s", "u", "v")), copying((2, 4), 2, down_pieces(1, TWO, down2))],
        "e": lambda: [copying((1, 4), 4, down_pieces(0, ALL, down0))],
    }
    for name, span in spans.items():
        (own, out, *results), t = back0(place, t, span, dhs, gate, up, aT0, w_down, beside[name]())
        copied(results, ("gate", "up", "down")[: len(results)] if name != "e" else ("down",))
        came = over(out, OVER_CORE)
        results, t = alone(place, t, (2 * span[2],), [into(0, span, own, came)])
        new0[name] = took(results, "into")

    here, there = slice(4), slice(4, None)
    for name, q, part in (("a", 4, slice(None)), ("c", 8, slice(None)), ("e", 4, here), ("e", 4, there)):
        pieces = list(into_pieces(0, spans[name], new0[name]))[part]
        grid = (len(pieces) // q + 2,)
        jobs = [copying(grid, q, pieces)]
        results, t = call(nothing, place, t, [], [], grid, jobs=jobs)
        copied(results, ("gate", "up", "down")[: len(results)])
    held, o_down = (weights_out["gate"], weights_out["up"]), weights_out["down"]
    (m_gate, m_up, v_gate, v_up), (m_down, v_down) = mv["into"], mv["down"]
    return *held, o_down, m_gate, m_up, m_down, v_gate, v_up, v_down


def solution(mesh):
    sequences, whole = P(("rep", "dp"), None, None), P(None, None, None)
    block, group, own = P(None, "dp", None), P("rep", None, None), P("rep", "dp", None)
    return jax.shard_map(
        whole_step,
        mesh=mesh,
        in_specs=(sequences,) * 2 + (whole,) * 3 + (block,) * 6,
        out_specs=(group,) * 3 + (own,) * 6,
        check_vma=False,
    )
```
